256 devices in a mesh: row: 16 (over x_hi, y, core), col: 16 (over z, x_lo).
Axes of the slice: x: 4 (x_hi: 2, x_lo: 2; x = x_hi * 2 + x_lo), y: 4, z: 8, core: 2. Of those that a mesh axis runs over, the one named last changes fastest.
Arguments:
- columns: float32 [16384, 16384], P('col', 'row'), may hold values from -64 to 64
- block_order: int32 [256], P('col'), may hold values from 0 to 255, as said below
Outputs:
- rotated: float32 [16384, 16384], P('col', 'row')
The draws below stay inside these ranges and needn't reach their ends.
Inputs may be any that keep to these rules, and one draw needn't show every extreme that they name: block_order is a permutation of 0 .. 255 in which slots c * 16 to (c + 1) * 16 - 1 name blocks c * 16 to (c + 1) * 16 - 1.
All inputs are finite; a program needn't handle non-finite values.
Results may differ from the reference program's by a relative error of at most 0.00055.
Values sent between devices are 32-bit elements; how exact they have to be, the bound alone decides.
A program may use at most 64 MiB of HBM per device.

```python
import math
import jax
import jax.numpy as jnp
from jax import lax

BLOCK = 64
STEPS = 4
BLOCKS_DEV = 16
N = 16384
M = 16384
BLOCKS = 256


def draw_columns(key, part):
    keys = jax.random.split(key, 4)
    gain_rows = 1.0 + 2.0 * jnp.arange(M, dtype=jnp.float32) / M
    loadings = jax.random.truncated_normal(keys[2], -3.0, 3.0, (N,), jnp.float32)
    noise = jax.random.truncated_normal(keys[0], -4.0, 4.0, (N, M), jnp.float32)
    scales = jnp.exp(jax.random.uniform(keys[1], (N,), jnp.float32, math.log(0.3), math.log(3.0)))
    common = jax.random.truncated_normal(keys[3], -3.0, 3.0, (M,), jnp.float32)
    return noise * scales[:, None] + loadings[:, None] * (common * gain_rows)[None, :]


def draw_block_order(key, part):
    groups = BLOCKS // BLOCKS_DEV
    scores = jax.random.randint(key, (groups, BLOCKS_DEV), 0, 1 << 20) * BLOCKS_DEV + jnp.arange(BLOCKS_DEV, dtype=jnp.int32)[None, :]
    shuffled = jnp.argsort(scores, axis=1, stable=True).astype(jnp.int32)
    return (shuffled + (jnp.arange(groups, dtype=jnp.int32) * BLOCKS_DEV)[:, None]).reshape(-1)


def setup_inputs(seed: int = 0) -> dict:
    splits = jax.random.split(jax.random.key(seed), 3)
    return {
        "columns": draw_columns(jax.random.fold_in(splits[2], 71), 0),
        "block_order": draw_block_order(jax.random.fold_in(splits[2], 71), 0),
    }


def cayley_turn(cross_sum, col_norms):
    highest = lax.Precision.HIGHEST
    top_norms = col_norms[:, :BLOCK][:, :, None]
    bottom_norms = col_norms[:, BLOCK:][:, None, :]
    spread = bottom_norms - top_norms
    radius = jnp.sqrt(spread * spread + 4.0 * cross_sum * cross_sum)
    scale_term = (top_norms + bottom_norms) / BLOCK
    coupling = 2.0 * cross_sum * spread / (spread * spread + 4.0 * cross_sum * cross_sum + jnp.abs(spread) * radius + scale_term * scale_term)
    identity = jnp.eye(BLOCK, dtype=jnp.float32)
    left_system = identity + jnp.einsum('pij,pkj->pik', coupling, coupling, precision=highest)
    right_system = identity + jnp.einsum('pji,pjk->pik', coupling, coupling, precision=highest)
    left_factor = jnp.linalg.cholesky(left_system)
    right_factor = jnp.linalg.cholesky(right_system)
    identities = jnp.broadcast_to(identity, coupling.shape)
    upper_half = jnp.concatenate([identities, coupling], axis=2)
    lower_half = jnp.concatenate([-jnp.transpose(coupling, (0, 2, 1)), identities], axis=2)

    def solve_one(factor, target):
        return jax.scipy.linalg.cho_solve((factor, True), target)
    upper_solved = jax.vmap(solve_one)(left_factor, upper_half)
    lower_solved = jax.vmap(solve_one)(right_factor, lower_half)
    solved = jnp.concatenate([upper_solved, lower_solved], axis=1)
    plus_skew = jnp.concatenate([upper_half, lower_half], axis=1)
    return jnp.einsum('pij,pjk->pik', plus_skew, solved, precision=highest)

def reference(columns, block_order):
    highest = lax.Precision.HIGHEST
    width, length = columns.shape
    count = width // BLOCK
    blocks = jnp.take(columns.reshape(count, BLOCK, length), block_order.astype(jnp.int32), axis=0)
    blocks = blocks.reshape(count // 2, 2 * BLOCK, length)
    for sweep_step in range(STEPS):
        gram_sum = jnp.einsum('pim,pjm->pij', blocks, blocks, precision=highest)
        col_norms = jnp.diagonal(gram_sum, axis1=1, axis2=2)
        cross_sum = gram_sum[:, :BLOCK, BLOCK:]
        turn_matrix = cayley_turn(cross_sum, col_norms)
        turned = jnp.einsum('pij,pim->pjm', turn_matrix, blocks, precision=highest)
        top_blocks = turned[:, :BLOCK]
        bottom_blocks = turned[:, BLOCK:]
        new_tops = jnp.concatenate([top_blocks[:1], bottom_blocks[:1], top_blocks[1:-1]], axis=0)
        new_bottoms = jnp.concatenate([bottom_blocks[1:], top_blocks[-1:]], axis=0)
        blocks = jnp.concatenate([new_tops, new_bottoms], axis=1)
    return blocks.reshape(width, length)
```

```python
import functools

import jax
import jax.numpy as jnp
from jax import lax
from jax.experimental import pallas as pl
from jax.experimental.pallas import tpu as pltpu
from jax.sharding import PartitionSpec as P

BLOCK = 64
PAIR = 2 * BLOCK
STEPS = 4
PAIRS = 8
ROWS = 16
COLS = 16
SOLVE_ITERS = 7
SPECTRUM_TOP = 372.0
MESSAGE = 40
HIGHEST = lax.Precision.HIGHEST
MESH = pl.DeviceIdType.MESH


def dot(a, b, dims=((1,), (0,))):
    return lax.dot_general(a, b, (dims, ((), ())), precision=HIGHEST, preferred_element_type=jnp.float32)


def iota(axis):
    return lax.broadcasted_iota(jnp.int32, (PAIR, PAIR), axis)


def solve_turn(message):
    folded = message[:32]
    cross = jnp.concatenate([pltpu.roll(folded, BLOCK, 1), folded], axis=0)
    norms = message[32:33]
    bottom_norms = jnp.broadcast_to(norms, (BLOCK, PAIR))
    top_norms = jnp.transpose(jnp.broadcast_to(norms, (PAIR, PAIR)))[:BLOCK]
    spread = bottom_norms - top_norms
    square = spread * spread + 4.0 * cross * cross
    radius = jnp.sqrt(square)
    scale_term = (top_norms + bottom_norms) / BLOCK
    coupling = 2.0 * cross * spread / (square + jnp.abs(spread) * radius + scale_term * scale_term)
    lane = lax.broadcasted_iota(jnp.int32, (BLOCK, PAIR), 1)
    upper = jnp.where(lane >= BLOCK, coupling, 0.0)
    upper = jnp.concatenate([upper, jnp.zeros_like(upper)], axis=0)
    skew = upper - jnp.transpose(upper)
    identity = (iota(0) == iota(1)).astype(jnp.float32)
    alpha = 2.0 / (1.0 + SPECTRUM_TOP)
    delta = (SPECTRUM_TOP - 1.0) / (SPECTRUM_TOP + 1.0)
    left = (1.0 - alpha) * identity + alpha * dot(skew, skew)
    result = alpha * (identity - skew)
    for step in range(SOLVE_ITERS):
        scale = 2.0 / (2.0 - delta * delta)
        delta = delta * delta / (2.0 - delta * delta)
        if step < SOLVE_ITERS - 1:
            both = dot(left, jnp.concatenate([left, result], axis=1))
            result = scale * (result + both[:, PAIR:])
            left = (1.0 - scale) * identity + scale * both[:, :PAIR]
        else:
            result = result + dot(left, result)
    rest = identity - result - dot(skew, result)
    result = result + dot(result, rest)
    return 2.0 * result - identity


def kernel(order_ref, x_hbm, out_hbm, xin, buf, gram, gram_in, turns, turn_left, turn_right,
           in_sem, out_sem, gram_send, gram_recv, turn_send, turn_recv, pass_send,
           edge_send, edge_recv, halo_send, halo_recv):
    row = lax.axis_index("row")
    col = lax.axis_index("col")
    chip = row // 2
    core = row % 2
    partner = 2 * chip + 1 - core
    owner = chip % 2 == core
    has_left = col > 0
    has_right = col < COLS - 1

    load = pltpu.make_async_copy(x_hbm, xin, in_sem)
    load.start()

    barrier = pltpu.get_barrier_semaphore()
    for other in range(1, ROWS):
        pl.semaphore_signal(barrier, inc=1, device_id={"row": (row + other) % ROWS, "col": col}, device_id_type=MESH)

    @pl.when(has_left)
    def _():
        pl.semaphore_signal(barrier, inc=1, device_id={"row": row, "col": col - 1}, device_id_type=MESH)

    @pl.when(has_right)
    def _():
        pl.semaphore_signal(barrier, inc=1, device_id={"row": row, "col": col + 1}, device_id_type=MESH)

    pl.semaphore_wait(barrier, ROWS - 1 + has_left.astype(jnp.int32) + has_right.astype(jnp.int32))

    load.wait()

    def place(slot):
        source = order_ref[slot] & (2 * PAIRS - 1)
        buf[0, pl.ds(PAIR + slot * BLOCK, BLOCK), :] = xin[source]

    def remote(src, dst, send, recv, row_to, col_to):
        return pltpu.make_async_remote_copy(
            src_ref=src, dst_ref=dst, send_sem=send, recv_sem=recv,
            device_id={"row": row_to, "col": col_to}, device_id_type=MESH,
        )

    def first_right():
        return remote(buf.at[0, pl.ds(PAIRS * PAIR, PAIR)], buf.at[0, pl.ds(0, PAIR)],
                      halo_send.at[0, 0], halo_recv.at[0, 0], row, col + 1)

    def first_left():
        return remote(buf.at[0, pl.ds(PAIR, PAIR)], buf.at[0, pl.ds((PAIRS + 1) * PAIR, PAIR)],
                      halo_send.at[0, 1], halo_recv.at[0, 1], row, col - 1)

    def halo_right(step):
        return remote(buf.at[step, pl.ds(16 * BLOCK, BLOCK)], buf.at[step, pl.ds(0, BLOCK)],
                      halo_send.at[step, 0], halo_recv.at[step, 0], row, col + 1)

    def halo_left(step):
        return remote(buf.at[step, pl.ds(3 * BLOCK, BLOCK)], buf.at[step, pl.ds(19 * BLOCK, BLOCK)],
                      halo_send.at[step, 1], halo_recv.at[step, 1], row, col - 1)

    def edge_right(step):
        return remote(turns.at[step, PAIRS - 1, pl.ds(0, BLOCK)], turn_left.at[step],
                      edge_send.at[step, 0], edge_recv.at[step, 0], row, col + 1)

    def edge_left(step):
        return remote(turns.at[step, 0, pl.ds(BLOCK, BLOCK)], turn_right.at[step],
                      edge_send.at[step, 1], edge_recv.at[step, 1], row, col - 1)

    def gram_out(step, pair):
        return remote(gram.at[step, pair], gram_in.at[step, row], gram_send.at[step, pair],
                      gram_recv.at[step, row], 2 * pair + pair % 2, col)

    def gram_from(step, source):
        return remote(gram.at[step, chip], gram_in.at[step, source], gram_send.at[step, 0],
                      gram_recv.at[step, source], source, col)

    def turn_out(step, other):
        return remote(turns.at[step, chip], turns.at[step, chip], turn_send.at[step, other],
                      turn_recv.at[step, chip], (row + 2 * other) % ROWS, col)

    def turn_pass(step, pair):
        return remote(turns.at[step, pair], turns.at[step, pair], pass_send.at[step, pair // 2],
                      turn_recv.at[step, pair], partner, col)

    for slot in (14, 15, 0, 1):
        place(slot)

    @pl.when(has_right)
    def _():
        first_right().start()

    @pl.when(has_left)
    def _():
        first_left().start()

    for slot in range(2, 14):
        place(slot)

    def make_gram(step, pair):
        start = pl.multiple_of((pair + 1) * PAIR, PAIR)
        both = buf[step, pl.ds(start, PAIR), :]
        cross = dot(both[:BLOCK], both[BLOCK:], ((1,), (1,)))
        gram[step, pair, :32, :] = jnp.concatenate([cross[:32], cross[32:]], axis=1)
        squares = both * both
        total = squares[:, :128]
        for piece in range(1, squares.shape[1] // 128):
            total = total + squares[:, piece * 128:(piece + 1) * 128]
        norms = jnp.sum(jnp.transpose(total), axis=0, keepdims=True)
        gram[step, pair, 32:, :] = jnp.broadcast_to(norms, (8, 128))

    def sum_and_solve(step):
        total = gram[step, chip]
        for other in range(1, ROWS):
            source = (row + other) % ROWS
            gram_from(step, source).wait_recv()
            total = total + gram_in[step, source]
        turns[step, chip] = solve_turn(total)

    def one_step(step, carry):
        def gram_body(pair, inner):
            make_gram(step, pair)

            @pl.when(2 * pair + pair % 2 != row)
            def _():
                gram_out(step, pair).start()
            return inner

        lax.fori_loop(0, PAIRS, gram_body, 0)

        @pl.when(owner)
        def _():
            sum_and_solve(step)
            for other in range(1, PAIRS):
                turn_out(step, other).start()

        def pass_body(index, inner):
            pair = 2 * ((index + chip // 2) % 4) + core

            @pl.when(pair != chip)
            def _():
                turn_pass(step, pair).wait_recv()
            turn_pass(step, pair).start()
            return inner

        lax.fori_loop(0, PAIRS // 2, pass_body, 0)

        def take_body(index, inner):
            turn_pass(step, 2 * index + 1 - core).wait_recv()
            return inner

        lax.fori_loop(0, PAIRS // 2, take_body, 0)

        @pl.when(has_right)
        def _():
            edge_right(step).start()

        @pl.when(has_left)
        def _():
            edge_left(step).start()

        at_first = col == 0
        at_last = col == COLS - 1

        def rows_of(slot):
            return pl.ds(pl.multiple_of(slot * BLOCK, BLOCK), BLOCK)

        def apply_body(pair, inner):
            start = pl.multiple_of((pair + 1) * PAIR, PAIR)
            turned = dot(turns[step, pair], buf[step, pl.ds(start, PAIR), :])
            corner = jnp.logical_and(pair == 0, at_first)
            far = jnp.logical_and(pair == PAIRS - 1, at_last)
            top_slot = jnp.where(corner, 2, jnp.where(far, 17, 2 * pair + 4))
            bottom_slot = jnp.where(corner, 4, 2 * pair + 1)
            buf[step + 1, rows_of(top_slot), :] = turned[:BLOCK]
            buf[step + 1, rows_of(bottom_slot), :] = turned[BLOCK:]
            return inner

        lax.fori_loop(0, PAIRS, apply_body, 0)

        @pl.when(jnp.logical_and(has_right, step < STEPS - 1))
        def _():
            halo_right(step + 1).start()

        @pl.when(jnp.logical_and(has_left, step < STEPS - 1))
        def _():
            halo_left(step + 1).start()

        @pl.when(has_left)
        def _():
            @pl.when(step == 0)
            def _():
                first_right().wait_recv()

            @pl.when(step > 0)
            def _():
                halo_right(step).wait_recv()
            edge_right(step).wait_recv()
            buf[step + 1, pl.ds(2 * BLOCK, BLOCK), :] = dot(turn_left[step], buf[step, pl.ds(0, PAIR), :])

        @pl.when(has_right)
        def _():
            @pl.when(step == 0)
            def _():
                first_left().wait_recv()

            @pl.when(step > 0)
            def _():
                halo_left(step).wait_recv()
            edge_left(step).wait_recv()
            buf[step + 1, pl.ds(17 * BLOCK, BLOCK), :] = dot(
                turn_right[step], buf[step, pl.ds((PAIRS + 1) * PAIR, PAIR), :]
            )
        return carry

    lax.fori_loop(0, STEPS, one_step, 0)

    store = pltpu.make_async_copy(buf.at[STEPS, pl.ds(PAIR, PAIRS * PAIR)], out_hbm, out_sem)
    store.start()

    def drain(step, carry):
        def drain_gram(pair, inner):
            @pl.when(2 * pair + pair % 2 != row)
            def _():
                gram_out(step, pair).wait_send()
            return inner

        lax.fori_loop(0, PAIRS, drain_gram, 0)

        @pl.when(owner)
        def _():
            for other in range(1, PAIRS):
                turn_out(step, other).wait_send()

        def drain_pass(index, inner):
            turn_pass(step, 2 * index + core).wait_send()
            return inner

        lax.fori_loop(0, PAIRS // 2, drain_pass, 0)

        @pl.when(has_right)
        def _():
            edge_right(step).wait_send()

            @pl.when(step == 0)
            def _():
                first_right().wait_send()

            @pl.when(step > 0)
            def _():
                halo_right(step).wait_send()

        @pl.when(has_left)
        def _():
            edge_left(step).wait_send()

            @pl.when(step == 0)
            def _():
                first_left().wait_send()

            @pl.when(step > 0)
            def _():
                halo_left(step).wait_send()
        return carry

    lax.fori_loop(0, STEPS, drain, 0)
    store.wait()


def local(columns, block_order):
    length = columns.shape[1]
    blocks = columns.reshape(2 * PAIRS, BLOCK, length)
    dma = pltpu.SemaphoreType.DMA
    return pl.pallas_call(
        kernel,
        out_shape=jax.ShapeDtypeStruct(columns.shape, jnp.float32),
        in_specs=[
            pl.BlockSpec(memory_space=pltpu.SMEM),
            pl.BlockSpec(memory_space=pl.ANY),
        ],
        out_specs=pl.BlockSpec(memory_space=pl.ANY),
        scratch_shapes=[
            pltpu.VMEM(blocks.shape, jnp.float32),
            pltpu.VMEM((STEPS + 1, (PAIRS + 2) * PAIR, length), jnp.float32),
            pltpu.VMEM((STEPS, PAIRS, MESSAGE, PAIR), jnp.float32),
            pltpu.VMEM((STEPS, ROWS, MESSAGE, PAIR), jnp.float32),
            pltpu.VMEM((STEPS, PAIRS, PAIR, PAIR), jnp.float32),
            pltpu.VMEM((STEPS, BLOCK, PAIR), jnp.float32),
            pltpu.VMEM((STEPS, BLOCK, PAIR), jnp.float32),
            dma,
            dma,
            dma((STEPS, PAIRS)),
            dma((STEPS, ROWS)),
            dma((STEPS, PAIRS)),
            dma((STEPS, PAIRS)),
            dma((STEPS, PAIRS // 2)),
            dma((STEPS, 2)),
            dma((STEPS, 2)),
            dma((STEPS, 2)),
            dma((STEPS, 2)),
        ],
        compiler_params=pltpu.CompilerParams(
            collective_id=0, has_side_effects=True, vmem_limit_bytes=60 * 1024 * 1024
        ),
    )(block_order, blocks)


def solution(mesh):
    placed = (P("col", "row"), P("col"))
    return jax.shard_map(
        local, mesh=mesh, in_specs=placed, out_specs=P("col", "row"), check_vma=False
    )
```

```python
import jax
import jax.numpy as jnp
from jax import lax
from jax.experimental import pallas as pl
from jax.experimental.pallas import tpu as pltpu
from jax.sharding import PartitionSpec as P

BLOCK = 64
PAIR = 2 * BLOCK
STEPS = 4
PAIRS = 8
ROWS = 16
COLS = 16
SLOTS = 2 * PAIRS + 4
SOLVE_ITERS = 7
SPECTRUM_TOP = 372.0
MESSAGE = 40
ORDER = (2, 3, 4, 5, 1, 6, 0, 7)
READY = {4: (3,), 5: (4,), 1: (2,), 6: (5,), 0: (1,), 7: (6,)}
FAR_FIRST = ((1, 2), (1, 1), (1, 3), (0, 2), (1, 0), (0, 1), (0, 3))
FIRST_CUTS = (0, 16, 64, 128)
LATER_CUTS = (0, 40, 64)
HIGHEST = lax.Precision.HIGHEST
MESH = pl.DeviceIdType.MESH


def dot(a, b, dims=((1,), (0,)), precision=None):
    return lax.dot_general(a, b, (dims, ((), ())), precision=precision, preferred_element_type=jnp.float32)


def pieces(value, count):
    parts = []
    for index in range(count):
        part = value.astype(jnp.bfloat16)
        parts.append(part)
        if index < count - 1:
            value = value - part.astype(jnp.float32)
    return parts


def turn_pieces(turn):
    return jnp.concatenate([jnp.concatenate([part, part], axis=1) for part in pieces(turn, 3)], axis=0)


def turned(stacked, block):
    rows = stacked.shape[0] // 3
    out = dot(stacked, jnp.concatenate(pieces(block, 2), axis=0))
    return out[:rows] + (out[rows : 2 * rows] + out[2 * rows :])


def iota(axis):
    return lax.broadcasted_iota(jnp.int32, (PAIR, PAIR), axis)


def solve_turn(message):
    folded = message[:32]
    cross = jnp.concatenate([pltpu.roll(folded, BLOCK, 1), folded], axis=0)
    norms = message[32:33]
    bottom_norms = jnp.broadcast_to(norms, (BLOCK, PAIR))
    top_norms = jnp.transpose(jnp.broadcast_to(norms, (PAIR, PAIR)))[:BLOCK]
    spread = bottom_norms - top_norms
    square = spread * spread + 4.0 * cross * cross
    radius = jnp.sqrt(square)
    scale_term = (top_norms + bottom_norms) / BLOCK
    coupling = 2.0 * cross * spread / (square + jnp.abs(spread) * radius + scale_term * scale_term)
    lane = lax.broadcasted_iota(jnp.int32, (BLOCK, PAIR), 1)
    upper = jnp.where(lane >= BLOCK, coupling, 0.0)
    upper = jnp.concatenate([upper, jnp.zeros_like(upper)], axis=0)
    skew = upper - jnp.transpose(upper)
    identity = (iota(0) == iota(1)).astype(jnp.float32)

    def product(left, right):
        high, low = pieces(left, 2)
        tall = jnp.concatenate(
            [jnp.concatenate([high, high], axis=1), jnp.concatenate([low, low], axis=1)], axis=0
        )
        both = dot(tall, jnp.concatenate(pieces(right, 2), axis=0))
        return both[:PAIR] + both[PAIR:]

    alpha = 2.0 / (1.0 + SPECTRUM_TOP)
    delta = (SPECTRUM_TOP - 1.0) / (SPECTRUM_TOP + 1.0)
    left = (1.0 - alpha) * identity + alpha * product(skew, skew)
    result = alpha * (identity - skew)
    for step in range(SOLVE_ITERS):
        scale = 2.0 / (2.0 - delta * delta)
        delta = delta * delta / (2.0 - delta * delta)
        if step < SOLVE_ITERS - 1:
            both = product(left, jnp.concatenate([left, result], axis=1))
            result = scale * (result + both[:, PAIR:])
            left = (1.0 - scale) * identity + scale * both[:, :PAIR]
        else:
            result = result + product(left, result)
    rest = identity - result - dot(skew, result, precision=HIGHEST)
    result = result + dot(result, rest, precision=HIGHEST)
    return 2.0 * result - identity


def make_gram(both):
    top = jnp.concatenate(pieces(both[:BLOCK], 3), axis=0)
    bottom = jnp.concatenate(pieces(both[BLOCK:], 3), axis=0)
    out = dot(top, bottom, ((1,), (1,)))

    def term(i, j):
        return out[i * BLOCK : (i + 1) * BLOCK, j * BLOCK : (j + 1) * BLOCK]

    cross = term(0, 0) + ((term(0, 1) + term(1, 0)) + (term(1, 1) + (term(0, 2) + term(2, 0))))
    squares = both * both
    total = squares[:, :128]
    for piece in range(1, squares.shape[1] // 128):
        total = total + squares[:, piece * 128 : (piece + 1) * 128]
    norms = jnp.sum(jnp.transpose(total), axis=0, keepdims=True)
    return jnp.concatenate([cross[:32], cross[32:]], axis=1), jnp.broadcast_to(norms, (8, 128))


def sweep(order_ref, x_hbm, last_x, last_turns, last_edges, xin, buf, gram, gram_in, turns, edges,
          in_sem, out_sem, gram_send, gram_recv, turn_send, turn_recv, pass_send,
          edge_send, edge_recv, first_send, first_recv, halo_send, halo_recv):
    row = lax.axis_index("row")
    col = lax.axis_index("col")
    chip = row // 2
    core = row % 2
    partner = 2 * chip + 1 - core
    owner = chip % 2 == core
    has_left = col > 0
    has_right = col < COLS - 1
    at_first = col == 0
    at_last = col == COLS - 1

    load = pltpu.make_async_copy(x_hbm, xin, in_sem)
    load.start()

    barrier = pltpu.get_barrier_semaphore()
    for other in range(1, ROWS):
        pl.semaphore_signal(barrier, inc=1, device_id={"row": (row + other) % ROWS, "col": col}, device_id_type=MESH)

    @pl.when(has_left)
    def _():
        pl.semaphore_signal(barrier, inc=1, device_id={"row": row, "col": col - 1}, device_id_type=MESH)

    @pl.when(has_right)
    def _():
        pl.semaphore_signal(barrier, inc=1, device_id={"row": row, "col": col + 1}, device_id_type=MESH)

    pl.semaphore_wait(barrier, ROWS - 1 + has_left.astype(jnp.int32) + has_right.astype(jnp.int32))
    load.wait()

    def place(slot):
        source = order_ref[slot] & (2 * PAIRS - 1)
        buf[0, pl.ds(PAIR + slot * BLOCK, BLOCK), :] = xin[source]

    def remote(src, dst, send, recv, row_to, col_to):
        return pltpu.make_async_remote_copy(
            src_ref=src, dst_ref=dst, send_sem=send, recv_sem=recv,
            device_id={"row": row_to, "col": col_to}, device_id_type=MESH,
        )

    def first_right(cut):
        low, high = FIRST_CUTS[cut], FIRST_CUTS[cut + 1]
        return remote(buf.at[0, pl.ds(PAIRS * PAIR + low, high - low)], buf.at[0, pl.ds(low, high - low)],
                      first_send.at[0, cut], first_recv.at[0, cut], row, col + 1)

    def first_left(cut):
        low, high = FIRST_CUTS[cut], FIRST_CUTS[cut + 1]
        return remote(buf.at[0, pl.ds(PAIR + low, high - low)],
                      buf.at[0, pl.ds((PAIRS + 1) * PAIR + low, high - low)],
                      first_send.at[1, cut], first_recv.at[1, cut], row, col - 1)

    def halo_right(step, cut):
        low, high = LATER_CUTS[cut], LATER_CUTS[cut + 1]
        return remote(buf.at[step, pl.ds(16 * BLOCK + low, high - low)], buf.at[step, pl.ds(low, high - low)],
                      halo_send.at[step, cut], halo_recv.at[step, cut], row, col + 1)

    def halo_left(step, cut):
        low, high = LATER_CUTS[cut], LATER_CUTS[cut + 1]
        return remote(buf.at[step, pl.ds(3 * BLOCK + low, high - low)],
                      buf.at[step, pl.ds(19 * BLOCK + low, high - low)],
                      halo_send.at[step, 2 + cut], halo_recv.at[step, 2 + cut], row, col - 1)

    def edge_right(step):
        return remote(turns.at[step, PAIRS - 1, pl.ds(0, BLOCK)], edges.at[step, 0],
                      edge_send.at[step, 0], edge_recv.at[step, 0], row, col + 1)

    def edge_left(step):
        return remote(turns.at[step, 0, pl.ds(BLOCK, BLOCK)], edges.at[step, 1],
                      edge_send.at[step, 1], edge_recv.at[step, 1], row, col - 1)

    def gram_out(step, pair):
        return remote(gram.at[step, pair], gram_in.at[step, row], gram_send.at[step, pair],
                      gram_recv.at[step, row], 2 * pair + pair % 2, col)

    def gram_from(step, source):
        return remote(gram.at[step, chip], gram_in.at[step, source], gram_send.at[step, 0],
                      gram_recv.at[step, source], source, col)

    def turn_out(step, index):
        far, along = FAR_FIRST[index]
        chip_to = (chip // 4 + far) % 2 * 4 + (chip % 4 + along) % 4
        return remote(turns.at[step, chip], turns.at[step, chip], turn_send.at[step, index],
                      turn_recv.at[step, chip], 2 * chip_to + core, col)

    def turn_pass(step, pair):
        return remote(turns.at[step, pair], turns.at[step, pair], pass_send.at[step, pair],
                      turn_recv.at[step, pair], partner, col)

    def send_gram(step, pair):
        folded, norms = make_gram(buf[step, pl.ds((pair + 1) * PAIR, PAIR), :])
        gram[step, pair, :32, :] = folded
        gram[step, pair, 32:, :] = norms

        @pl.when(row != 2 * pair + pair % 2)
        def _():
            gram_out(step, pair).start()

    def sides(right, left):
        pl.when(has_right)(right)
        pl.when(has_left)(left)

    def solve_and_send(step):
        @pl.when(owner)
        def _():
            total = gram[step, chip]
            for other in range(1, ROWS):
                source = (row + other) % ROWS
                gram_from(step, source).wait_recv()
                total = total + gram_in[step, source]
            turns[step, chip] = solve_turn(total)
            for index in range(len(FAR_FIRST)):
                turn_out(step, index).start()

    def take_turn(step, pair):
        @pl.when(row != 2 * pair + pair % 2)
        def _():
            turn_pass(step, pair).wait_recv()

        @pl.when(core == pair % 2)
        def _():
            turn_pass(step, pair).start()

        if pair == PAIRS - 1:
            pl.when(has_right)(lambda: edge_right(step).start())
        if pair == 0:
            pl.when(has_left)(lambda: edge_left(step).start())

    def rows_of(slot):
        return pl.ds(pl.multiple_of(slot * BLOCK, BLOCK), BLOCK)

    for slot in (14, 15, 0, 1):
        place(slot)
    sides(lambda: first_right(0).start(), lambda: first_left(0).start())
    for pair in (7, 0) + tuple(range(1, PAIRS - 1)):
        if pair not in (0, PAIRS - 1):
            place(2 * pair)
            place(2 * pair + 1)
        send_gram(0, pair)
    sides(lambda: first_right(1).start(), lambda: first_left(1).start())

    def one_step(step, carry):
        solve_and_send(step)

        @pl.when(step == 0)
        def _():
            sides(lambda: first_right(2).start(), lambda: first_left(2).start())

        @pl.when(step > 0)
        def _():
            sides(lambda: halo_right(step, 1).start(), lambda: halo_left(step, 1).start())

        for pair in ORDER:
            take_turn(step, pair)
            out = turned(turn_pieces(turns[step, pair]), buf[step, pl.ds((pair + 1) * PAIR, PAIR), :])
            top_slot, bottom_slot = 2 * pair + 4, 2 * pair + 1
            if pair == 0:
                top_slot = jnp.where(at_first, 2, top_slot)
                bottom_slot = jnp.where(at_first, 4, bottom_slot)
            if pair == PAIRS - 1:
                top_slot = jnp.where(at_last, 17, top_slot)
            buf[step + 1, rows_of(top_slot), :] = out[:BLOCK]
            buf[step + 1, rows_of(bottom_slot), :] = out[BLOCK:]
            for ready in READY.get(pair, ()):
                send_gram(step + 1, ready)

        @pl.when(has_left)
        def _():
            @pl.when(step == 0)
            def _():
                for cut in range(len(FIRST_CUTS) - 1):
                    first_right(cut).wait_recv()

            @pl.when(step > 0)
            def _():
                for cut in range(len(LATER_CUTS) - 1):
                    halo_right(step, cut).wait_recv()
            edge_right(step).wait_recv()
            buf[step + 1, pl.ds(2 * BLOCK, BLOCK), :] = turned(
                turn_pieces(edges[step, 0]), buf[step, pl.ds(0, PAIR), :]
            )

        send_gram(step + 1, 0)

        @pl.when(has_right)
        def _():
            @pl.when(step == 0)
            def _():
                for cut in range(len(FIRST_CUTS) - 1):
                    first_left(cut).wait_recv()

            @pl.when(step > 0)
            def _():
                for cut in range(len(LATER_CUTS) - 1):
                    halo_left(step, cut).wait_recv()
            edge_left(step).wait_recv()
            buf[step + 1, pl.ds(17 * BLOCK, BLOCK), :] = turned(
                turn_pieces(edges[step, 1]), buf[step, pl.ds((PAIRS + 1) * PAIR, PAIR), :]
            )

        send_gram(step + 1, PAIRS - 1)
        sides(lambda: halo_right(step + 1, 0).start(), lambda: halo_left(step + 1, 0).start())
        return carry

    lax.fori_loop(0, STEPS - 1, one_step, 0)

    last = STEPS - 1
    inner = pl.ds(BLOCK, (SLOTS - 2) * BLOCK)
    store_inner = pltpu.make_async_copy(buf.at[last, inner], last_x.at[inner], out_sem.at[0])
    store_inner.start()
    solve_and_send(last)
    sides(lambda: halo_right(last, 1).start(), lambda: halo_left(last, 1).start())
    for pair in ORDER[::-1]:
        take_turn(last, pair)
    store_turns = pltpu.make_async_copy(turns.at[last], last_turns, out_sem.at[1])
    store_turns.start()

    def store_side(side):
        rows = pl.ds(side * (SLOTS - 1) * BLOCK, BLOCK)
        return (
            pltpu.make_async_copy(buf.at[last, rows], last_x.at[rows], out_sem.at[2 + side]),
            pltpu.make_async_copy(edges.at[last, side], last_edges.at[side], out_sem.at[4 + side]),
        )

    @pl.when(has_left)
    def _():
        for cut in range(len(LATER_CUTS) - 1):
            halo_right(last, cut).wait_recv()
        edge_right(last).wait_recv()
        for copy in store_side(0):
            copy.start()

    @pl.when(has_right)
    def _():
        for cut in range(len(LATER_CUTS) - 1):
            halo_left(last, cut).wait_recv()
        edge_left(last).wait_recv()
        for copy in store_side(1):
            copy.start()

    def drain(step, carry):
        for pair in range(PAIRS):
            @pl.when(row != 2 * pair + pair % 2)
            def _():
                gram_out(step, pair).wait_send()

            @pl.when(core == pair % 2)
            def _():
                turn_pass(step, pair).wait_send()

        @pl.when(owner)
        def _():
            for index in range(len(FAR_FIRST)):
                turn_out(step, index).wait_send()

        sides(lambda: edge_right(step).wait_send(), lambda: edge_left(step).wait_send())

        @pl.when(step > 0)
        def _():
            for cut in range(len(LATER_CUTS) - 1):
                sides(lambda: halo_right(step, cut).wait_send(), lambda: halo_left(step, cut).wait_send())
        return carry

    lax.fori_loop(0, STEPS, drain, 0)
    for cut in range(len(FIRST_CUTS) - 1):
        sides(lambda: first_right(cut).wait_send(), lambda: first_left(cut).wait_send())
    store_inner.wait()
    store_turns.wait()

    @pl.when(has_left)
    def _():
        for copy in store_side(0):
            copy.wait()

    @pl.when(has_right)
    def _():
        for copy in store_side(1):
            copy.wait()


def finish(position, x_ref, turns_ref, edges_ref, out_ref):
    at_first = position[0] == 0
    at_last = position[0] == COLS - 1

    def put(slot, value):
        out_ref[slot * BLOCK : (slot + 1) * BLOCK, :] = value

    for pair in range(PAIRS):
        out = turned(turn_pieces(turns_ref[pair]), x_ref[(pair + 1) * PAIR : (pair + 2) * PAIR, :])
        top, bottom = out[:BLOCK], out[BLOCK:]
        if pair == 0:
            left = turned(turn_pieces(edges_ref[0]), x_ref[:PAIR, :])
            put(0, jnp.where(at_first, top, left))
            put(2, jnp.where(at_first, bottom, top))
        elif pair == PAIRS - 1:
            right = turned(turn_pieces(edges_ref[1]), x_ref[(PAIRS + 1) * PAIR :, :])
            put(2 * pair - 1, bottom)
            put(2 * pair + 1, jnp.where(at_last, top, right))
        else:
            put(2 * pair - 1, bottom)
            put(2 * pair + 2, top)


def local(columns, block_order):
    length = columns.shape[1]
    blocks = columns.reshape(2 * PAIRS, BLOCK, length)
    dma = pltpu.SemaphoreType.DMA
    position = lax.axis_index("col").astype(jnp.int32).reshape(1)
    last_x, last_turns, last_edges = pl.pallas_call(
        sweep,
        out_shape=(
            jax.ShapeDtypeStruct((SLOTS * BLOCK, length), jnp.float32),
            jax.ShapeDtypeStruct((PAIRS, PAIR, PAIR), jnp.float32),
            jax.ShapeDtypeStruct((2, BLOCK, PAIR), jnp.float32),
        ),
        in_specs=[
            pl.BlockSpec(memory_space=pltpu.SMEM),
            pl.BlockSpec(memory_space=pl.ANY),
        ],
        out_specs=(pl.BlockSpec(memory_space=pl.ANY),) * 3,
        scratch_shapes=[
            pltpu.VMEM(blocks.shape, jnp.float32),
            pltpu.VMEM((STEPS, SLOTS * BLOCK, length), jnp.float32),
            pltpu.VMEM((STEPS, PAIRS, MESSAGE, PAIR), jnp.float32),
            pltpu.VMEM((STEPS, ROWS, MESSAGE, PAIR), jnp.float32),
            pltpu.VMEM((STEPS, PAIRS, PAIR, PAIR), jnp.float32),
            pltpu.VMEM((STEPS, 2, BLOCK, PAIR), jnp.float32),
            dma,
            dma((6,)),
            dma((STEPS, PAIRS)),
            dma((STEPS, ROWS)),
            dma((STEPS, len(FAR_FIRST))),
            dma((STEPS, PAIRS)),
            dma((STEPS, PAIRS)),
            dma((STEPS, 2)),
            dma((STEPS, 2)),
            dma((2, len(FIRST_CUTS) - 1)),
            dma((2, len(FIRST_CUTS) - 1)),
            dma((STEPS, 2 * len(LATER_CUTS) - 2)),
            dma((STEPS, 2 * len(LATER_CUTS) - 2)),
        ],
        compiler_params=pltpu.CompilerParams(
            collective_id=0, has_side_effects=True, vmem_limit_bytes=58 * 1024 * 1024
        ),
    )(block_order, blocks)
    wide = 256
    return pl.pallas_call(
        finish,
        grid=(length // wide,),
        out_shape=jax.ShapeDtypeStruct(columns.shape, jnp.float32),
        in_specs=[
            pl.BlockSpec(memory_space=pltpu.SMEM),
            pl.BlockSpec((SLOTS * BLOCK, wide), lambda part: (0, part)),
            pl.BlockSpec((PAIRS, PAIR, PAIR), lambda part: (0, 0, 0)),
            pl.BlockSpec((2, BLOCK, PAIR), lambda part: (0, 0, 0)),
        ],
        out_specs=pl.BlockSpec((columns.shape[0], wide), lambda part: (0, part)),
    )(position, last_x, last_turns, last_edges)


def solution(mesh):
    placed = (P("col", "row"), P("col"))
    return jax.shard_map(
        local, mesh=mesh, in_specs=placed, out_specs=P("col", "row"), check_vma=False
    )
```

```python
import jax
import jax.numpy as jnp
from jax import lax
from jax.experimental import pallas as pl
from jax.experimental.pallas import tpu as pltpu
from jax.sharding import PartitionSpec as P

BLOCK = 64
PAIR = 2 * BLOCK
STEPS = 4
PAIRS = 8
ROWS = 16
COLS = 16
SLOTS = 2 * PAIRS + 4
SOLVE_ITERS = 7
SPECTRUM_TOP = 372.0
MESSAGE = 40
ORDER = (2, 3, 4, 5, 1, 6, 0, 7)
READY = {4: (3,), 5: (4,), 1: (2,), 6: (5,), 0: (1,), 7: (6,)}
FAR_FIRST = (2, 1, 3)
FIRST_CUTS = (0, 32, 88, 128)
LATER_CUTS = (0, 40, 64)
MESH = pl.DeviceIdType.MESH


def dot(a, b, dims=((1,), (0,))):
    return lax.dot_general(a, b, (dims, ((), ())), preferred_element_type=jnp.float32)


def pieces(value, count):
    parts = []
    for index in range(count):
        part = value.astype(jnp.bfloat16)
        parts.append(part)
        if index < count - 1:
            value = value - part.astype(jnp.float32)
    return parts


def turn_pieces(turn):
    return jnp.concatenate([jnp.concatenate([part, part], axis=1) for part in pieces(turn, 3)], axis=0)


def turned(stacked, block):
    rows = stacked.shape[0] // 3
    out = dot(stacked, jnp.concatenate(pieces(block, 2), axis=0))
    return out[:rows] + (out[rows : 2 * rows] + out[2 * rows :])


def fine_product(left, right):
    out = dot(jnp.concatenate(pieces(left, 3), axis=0), jnp.concatenate(pieces(right, 3), axis=1))

    def term(i, j):
        return out[i * PAIR : (i + 1) * PAIR, j * PAIR : (j + 1) * PAIR]

    return term(0, 0) + ((term(0, 1) + term(1, 0)) + (term(1, 1) + (term(0, 2) + term(2, 0))))


def iota(axis):
    return lax.broadcasted_iota(jnp.int32, (PAIR, PAIR), axis)


def solve_turn(message):
    folded = message[:32]
    cross = jnp.concatenate([pltpu.roll(folded, BLOCK, 1), folded], axis=0)
    norms = message[32:33]
    bottom_norms = jnp.broadcast_to(norms, (BLOCK, PAIR))
    top_norms = jnp.transpose(jnp.broadcast_to(norms, (PAIR, PAIR)))[:BLOCK]
    spread = bottom_norms - top_norms
    square = spread * spread + 4.0 * cross * cross
    radius = jnp.sqrt(square)
    scale_term = (top_norms + bottom_norms) / BLOCK
    coupling = 2.0 * cross * spread / (square + jnp.abs(spread) * radius + scale_term * scale_term)
    lane = lax.broadcasted_iota(jnp.int32, (BLOCK, PAIR), 1)
    upper = jnp.where(lane >= BLOCK, coupling, 0.0)
    upper = jnp.concatenate([upper, jnp.zeros_like(upper)], axis=0)
    skew = upper - jnp.transpose(upper)
    identity = (iota(0) == iota(1)).astype(jnp.float32)

    def product(left, right):
        high, low = pieces(left, 2)
        tall = jnp.concatenate(
            [jnp.concatenate([high, high], axis=1), jnp.concatenate([low, low], axis=1)], axis=0
        )
        both = dot(tall, jnp.concatenate(pieces(right, 2), axis=0))
        return both[:PAIR] + both[PAIR:]

    alpha = 2.0 / (1.0 + SPECTRUM_TOP)
    delta = (SPECTRUM_TOP - 1.0) / (SPECTRUM_TOP + 1.0)
    left = (1.0 - alpha) * identity + alpha * product(skew, skew)
    result = alpha * (identity - skew)
    for step in range(SOLVE_ITERS):
        scale = 2.0 / (2.0 - delta * delta)
        delta = delta * delta / (2.0 - delta * delta)
        if step < SOLVE_ITERS - 1:
            both = product(left, jnp.concatenate([left, result], axis=1))
            result = scale * (result + both[:, PAIR:])
            left = (1.0 - scale) * identity + scale * both[:, :PAIR]
        else:
            result = result + product(left, result)
    rest = identity - result - fine_product(skew, result)
    result = result + fine_product(result, rest)
    return 2.0 * result - identity


def make_gram(both):
    top = jnp.concatenate(pieces(both[:BLOCK], 3), axis=0)
    bottom = jnp.concatenate(pieces(both[BLOCK:], 3), axis=0)
    out = dot(top, bottom, ((1,), (1,)))

    def term(i, j):
        return out[i * BLOCK : (i + 1) * BLOCK, j * BLOCK : (j + 1) * BLOCK]

    cross = term(0, 0) + ((term(0, 1) + term(1, 0)) + (term(1, 1) + (term(0, 2) + term(2, 0))))
    squares = both * both
    total = squares[:, :128]
    for piece in range(1, squares.shape[1] // 128):
        total = total + squares[:, piece * 128 : (piece + 1) * 128]
    norms = jnp.sum(jnp.transpose(total), axis=0, keepdims=True)
    return jnp.concatenate([cross[:32], cross[32:]], axis=1), jnp.broadcast_to(norms, (8, 128))


def sweep(order_ref, x_hbm, last_x, last_turns, last_edges, xin, buf, gram, gram_in, half_sum, half_in,
          turns, edges, in_sem, out_sem, gram_send, gram_recv, swap_send, swap_recv, turn_send, turn_recv, pass_send,
          edge_send, edge_recv, first_send, first_recv, halo_send, halo_recv):
    row = lax.axis_index("row")
    col = lax.axis_index("col")
    half = row // PAIRS
    mine = row % PAIRS
    core = row % 2
    partner = row + 1 - 2 * core
    opposite = (row + PAIRS) % ROWS
    has_left = col > 0
    has_right = col < COLS - 1
    at_first = col == 0
    at_last = col == COLS - 1

    load = pltpu.make_async_copy(x_hbm, xin, in_sem)
    load.start()

    barrier = pltpu.get_barrier_semaphore()
    for other in range(1, PAIRS):
        near = half * PAIRS + (mine + other) % PAIRS
        pl.semaphore_signal(barrier, inc=1, device_id={"row": near, "col": col}, device_id_type=MESH)
    pl.semaphore_signal(barrier, inc=1, device_id={"row": opposite, "col": col}, device_id_type=MESH)

    @pl.when(has_left)
    def _():
        pl.semaphore_signal(barrier, inc=1, device_id={"row": row, "col": col - 1}, device_id_type=MESH)

    @pl.when(has_right)
    def _():
        pl.semaphore_signal(barrier, inc=1, device_id={"row": row, "col": col + 1}, device_id_type=MESH)

    pl.semaphore_wait(barrier, PAIRS + has_left.astype(jnp.int32) + has_right.astype(jnp.int32))
    load.wait()

    def place(slot):
        source = order_ref[slot] & (2 * PAIRS - 1)
        buf[0, pl.ds(PAIR + slot * BLOCK, BLOCK), :] = xin[source]

    def remote(src, dst, send, recv, row_to, col_to):
        return pltpu.make_async_remote_copy(
            src_ref=src, dst_ref=dst, send_sem=send, recv_sem=recv,
            device_id={"row": row_to, "col": col_to}, device_id_type=MESH,
        )

    def first_right(cut):
        low, high = FIRST_CUTS[cut], FIRST_CUTS[cut + 1]
        return remote(buf.at[0, pl.ds(PAIRS * PAIR + low, high - low)], buf.at[0, pl.ds(low, high - low)],
                      first_send.at[0, cut], first_recv.at[0, cut], row, col + 1)

    def first_left(cut):
        low, high = FIRST_CUTS[cut], FIRST_CUTS[cut + 1]
        return remote(buf.at[0, pl.ds(PAIR + low, high - low)],
                      buf.at[0, pl.ds((PAIRS + 1) * PAIR + low, high - low)],
                      first_send.at[1, cut], first_recv.at[1, cut], row, col - 1)

    def halo_right(step, cut):
        low, high = LATER_CUTS[cut], LATER_CUTS[cut + 1]
        return remote(buf.at[step, pl.ds(16 * BLOCK + low, high - low)], buf.at[step, pl.ds(low, high - low)],
                      halo_send.at[step, cut], halo_recv.at[step, cut], row, col + 1)

    def halo_left(step, cut):
        low, high = LATER_CUTS[cut], LATER_CUTS[cut + 1]
        return remote(buf.at[step, pl.ds(3 * BLOCK + low, high - low)],
                      buf.at[step, pl.ds(19 * BLOCK + low, high - low)],
                      halo_send.at[step, 2 + cut], halo_recv.at[step, 2 + cut], row, col - 1)

    def edge_right(step):
        return remote(turns.at[step, PAIRS - 1, pl.ds(0, BLOCK)], edges.at[step, 0],
                      edge_send.at[step, 0], edge_recv.at[step, 0], row, col + 1)

    def edge_left(step):
        return remote(turns.at[step, 0, pl.ds(BLOCK, BLOCK)], edges.at[step, 1],
                      edge_send.at[step, 1], edge_recv.at[step, 1], row, col - 1)

    def gram_out(step, pair):
        return remote(gram.at[step, pair], gram_in.at[step, mine], gram_send.at[step, pair],
                      gram_recv.at[step, mine], half * PAIRS + pair, col)

    def gram_from(step, source):
        return remote(gram.at[step, mine], gram_in.at[step, source], gram_send.at[step, 0],
                      gram_recv.at[step, source], half * PAIRS + source, col)

    def swap(step):
        return remote(half_sum.at[step], half_in.at[step], swap_send.at[step], swap_recv.at[step], opposite, col)

    def turn_out(step, index):
        along = (mine + 2 * FAR_FIRST[index]) % PAIRS
        return remote(turns.at[step, mine], turns.at[step, mine], turn_send.at[step, index],
                      turn_recv.at[step, mine], half * PAIRS + along, col)

    def turn_pass(step, pair):
        return remote(turns.at[step, pair], turns.at[step, pair], pass_send.at[step, pair],
                      turn_recv.at[step, pair], partner, col)

    def send_gram(step, pair):
        folded, norms = make_gram(buf[step, pl.ds((pair + 1) * PAIR, PAIR), :])
        gram[step, pair, :32, :] = folded
        gram[step, pair, 32:, :] = norms

        @pl.when(mine != pair)
        def _():
            gram_out(step, pair).start()

    def sides(right, left):
        pl.when(has_right)(right)
        pl.when(has_left)(left)

    def solve_and_send(step):
        total = gram[step, mine]
        for other in range(1, PAIRS):
            source = (mine + other) % PAIRS
            gram_from(step, source).wait_recv()
            total = total + gram_in[step, source]
        half_sum[step] = total
        swap(step).start()

        @pl.when(step == 0)
        def _():
            sides(lambda: first_right(1).start(), lambda: first_left(1).start())

        @pl.when(step > 0)
        def _():
            sides(lambda: halo_right(step, 1).start(), lambda: halo_left(step, 1).start())

        swap(step).wait_recv()
        turns[step, mine] = solve_turn(total + half_in[step])
        for index in range(len(FAR_FIRST)):
            turn_out(step, index).start()

    def take_turn(step, pair):
        @pl.when(mine != pair)
        def _():
            turn_pass(step, pair).wait_recv()

        @pl.when(core == pair % 2)
        def _():
            turn_pass(step, pair).start()

        if pair == PAIRS - 1:
            pl.when(has_right)(lambda: edge_right(step).start())
        if pair == 0:
            pl.when(has_left)(lambda: edge_left(step).start())

    def rows_of(slot):
        return pl.ds(pl.multiple_of(slot * BLOCK, BLOCK), BLOCK)

    for slot in (14, 15, 0, 1):
        place(slot)
    sides(lambda: first_right(0).start(), lambda: first_left(0).start())
    for pair in (7, 0) + tuple(range(1, PAIRS - 1)):
        if pair not in (0, PAIRS - 1):
            place(2 * pair)
            place(2 * pair + 1)
        send_gram(0, pair)

    def one_step(step, carry):
        solve_and_send(step)
        for pair in ORDER:
            take_turn(step, pair)
            out = turned(turn_pieces(turns[step, pair]), buf[step, pl.ds((pair + 1) * PAIR, PAIR), :])
            top_slot, bottom_slot = 2 * pair + 4, 2 * pair + 1
            if pair == 0:
                top_slot = jnp.where(at_first, 2, top_slot)
                bottom_slot = jnp.where(at_first, 4, bottom_slot)
            if pair == PAIRS - 1:
                top_slot = jnp.where(at_last, 17, top_slot)
            buf[step + 1, rows_of(top_slot), :] = out[:BLOCK]
            buf[step + 1, rows_of(bottom_slot), :] = out[BLOCK:]
            for ready in READY.get(pair, ()):
                send_gram(step + 1, ready)

        @pl.when(step == 0)
        def _():
            sides(lambda: first_right(2).start(), lambda: first_left(2).start())

        sides(lambda: halo_right(step + 1, 0).start(), lambda: halo_left(step + 1, 0).start())

        @pl.when(has_left)
        def _():
            @pl.when(step == 0)
            def _():
                for cut in range(len(FIRST_CUTS) - 1):
                    first_right(cut).wait_recv()

            @pl.when(step > 0)
            def _():
                for cut in range(len(LATER_CUTS) - 1):
                    halo_right(step, cut).wait_recv()
            edge_right(step).wait_recv()
            buf[step + 1, pl.ds(2 * BLOCK, BLOCK), :] = turned(
                turn_pieces(edges[step, 0]), buf[step, pl.ds(0, PAIR), :]
            )

        send_gram(step + 1, 0)

        @pl.when(has_right)
        def _():
            @pl.when(step == 0)
            def _():
                for cut in range(len(FIRST_CUTS) - 1):
                    first_left(cut).wait_recv()

            @pl.when(step > 0)
            def _():
                for cut in range(len(LATER_CUTS) - 1):
                    halo_left(step, cut).wait_recv()
            edge_left(step).wait_recv()
            buf[step + 1, pl.ds(17 * BLOCK, BLOCK), :] = turned(
                turn_pieces(edges[step, 1]), buf[step, pl.ds((PAIRS + 1) * PAIR, PAIR), :]
            )

        send_gram(step + 1, PAIRS - 1)
        return carry

    lax.fori_loop(0, STEPS - 1, one_step, 0)

    last = STEPS - 1
    inner = pl.ds(BLOCK, (SLOTS - 2) * BLOCK)
    store_inner = pltpu.make_async_copy(buf.at[last, inner], last_x.at[inner], out_sem.at[0])
    store_inner.start()
    solve_and_send(last)
    for pair in ORDER[::-1]:
        take_turn(last, pair)
    store_turns = pltpu.make_async_copy(turns.at[last], last_turns, out_sem.at[1])
    store_turns.start()

    def store_side(side):
        rows = pl.ds(side * (SLOTS - 1) * BLOCK, BLOCK)
        return (
            pltpu.make_async_copy(buf.at[last, rows], last_x.at[rows], out_sem.at[2 + side]),
            pltpu.make_async_copy(edges.at[last, side], last_edges.at[side], out_sem.at[4 + side]),
        )

    @pl.when(has_left)
    def _():
        for cut in range(len(LATER_CUTS) - 1):
            halo_right(last, cut).wait_recv()
        edge_right(last).wait_recv()
        for copy in store_side(0):
            copy.start()

    @pl.when(has_right)
    def _():
        for cut in range(len(LATER_CUTS) - 1):
            halo_left(last, cut).wait_recv()
        edge_left(last).wait_recv()
        for copy in store_side(1):
            copy.start()

    def drain(step, carry):
        for pair in range(PAIRS):
            @pl.when(mine != pair)
            def _():
                gram_out(step, pair).wait_send()

            @pl.when(core == pair % 2)
            def _():
                turn_pass(step, pair).wait_send()

        swap(step).wait_send()
        for index in range(len(FAR_FIRST)):
            turn_out(step, index).wait_send()

        sides(lambda: edge_right(step).wait_send(), lambda: edge_left(step).wait_send())

        @pl.when(step > 0)
        def _():
            for cut in range(len(LATER_CUTS) - 1):
                sides(lambda: halo_right(step, cut).wait_send(), lambda: halo_left(step, cut).wait_send())
        return carry

    lax.fori_loop(0, STEPS, drain, 0)
    for cut in range(len(FIRST_CUTS) - 1):
        sides(lambda: first_right(cut).wait_send(), lambda: first_left(cut).wait_send())
    store_inner.wait()
    store_turns.wait()

    @pl.when(has_left)
    def _():
        for copy in store_side(0):
            copy.wait()

    @pl.when(has_right)
    def _():
        for copy in store_side(1):
            copy.wait()


def finish(position, x_ref, turns_ref, edges_ref, out_ref):
    at_first = position[0] == 0
    at_last = position[0] == COLS - 1

    def put(slot, value):
        out_ref[slot * BLOCK : (slot + 1) * BLOCK, :] = value

    for pair in range(PAIRS):
        out = turned(turn_pieces(turns_ref[pair]), x_ref[(pair + 1) * PAIR : (pair + 2) * PAIR, :])
        top, bottom = out[:BLOCK], out[BLOCK:]
        if pair == 0:
            left = turned(turn_pieces(edges_ref[0]), x_ref[:PAIR, :])
            put(0, jnp.where(at_first, top, left))
            put(2, jnp.where(at_first, bottom, top))
        elif pair == PAIRS - 1:
            right = turned(turn_pieces(edges_ref[1]), x_ref[(PAIRS + 1) * PAIR :, :])
            put(2 * pair - 1, bottom)
            put(2 * pair + 1, jnp.where(at_last, top, right))
        else:
            put(2 * pair - 1, bottom)
            put(2 * pair + 2, top)


def local(columns, block_order):
    length = columns.shape[1]
    blocks = columns.reshape(2 * PAIRS, BLOCK, length)
    dma = pltpu.SemaphoreType.DMA
    position = lax.axis_index("col").astype(jnp.int32).reshape(1)
    last_x, last_turns, last_edges = pl.pallas_call(
        sweep,
        out_shape=(
            jax.ShapeDtypeStruct((SLOTS * BLOCK, length), jnp.float32),
            jax.ShapeDtypeStruct((PAIRS, PAIR, PAIR), jnp.float32),
            jax.ShapeDtypeStruct((2, BLOCK, PAIR), jnp.float32),
        ),
        in_specs=[
            pl.BlockSpec(memory_space=pltpu.SMEM),
            pl.BlockSpec(memory_space=pl.ANY),
        ],
        out_specs=(pl.BlockSpec(memory_space=pl.ANY),) * 3,
        scratch_shapes=[
            pltpu.VMEM(blocks.shape, jnp.float32),
            pltpu.VMEM((STEPS, SLOTS * BLOCK, length), jnp.float32),
            pltpu.VMEM((STEPS, PAIRS, MESSAGE, PAIR), jnp.float32),
            pltpu.VMEM((STEPS, PAIRS, MESSAGE, PAIR), jnp.float32),
            pltpu.VMEM((STEPS, MESSAGE, PAIR), jnp.float32),
            pltpu.VMEM((STEPS, MESSAGE, PAIR), jnp.float32),
            pltpu.VMEM((STEPS, PAIRS, PAIR, PAIR), jnp.float32),
            pltpu.VMEM((STEPS, 2, BLOCK, PAIR), jnp.float32),
            dma,
            dma((6,)),
            dma((STEPS, PAIRS)),
            dma((STEPS, PAIRS)),
            dma((STEPS,)),
            dma((STEPS,)),
            dma((STEPS, len(FAR_FIRST))),
            dma((STEPS, PAIRS)),
            dma((STEPS, PAIRS)),
            dma((STEPS, 2)),
            dma((STEPS, 2)),
            dma((2, len(FIRST_CUTS) - 1)),
            dma((2, len(FIRST_CUTS) - 1)),
            dma((STEPS, 2 * len(LATER_CUTS) - 2)),
            dma((STEPS, 2 * len(LATER_CUTS) - 2)),
        ],
        compiler_params=pltpu.CompilerParams(
            collective_id=0, has_side_effects=True, vmem_limit_bytes=58 * 1024 * 1024
        ),
    )(block_order, blocks)
    wide = 256
    return pl.pallas_call(
        finish,
        grid=(length // wide,),
        out_shape=jax.ShapeDtypeStruct(columns.shape, jnp.float32),
        in_specs=[
            pl.BlockSpec(memory_space=pltpu.SMEM),
            pl.BlockSpec((SLOTS * BLOCK, wide), lambda part: (0, part)),
            pl.BlockSpec((PAIRS, PAIR, PAIR), lambda part: (0, 0, 0)),
            pl.BlockSpec((2, BLOCK, PAIR), lambda part: (0, 0, 0)),
        ],
        out_specs=pl.BlockSpec((columns.shape[0], wide), lambda part: (0, part)),
    )(position, last_x, last_turns, last_edges)


def solution(mesh):
    placed = (P("col", "row"), P("col"))
    return jax.shard_map(
        local, mesh=mesh, in_specs=placed, out_specs=P("col", "row"), check_vma=False
    )
```

```python
import jax
import jax.numpy as jnp
from jax import lax
from jax.experimental import pallas as pl
from jax.experimental.pallas import tpu as pltpu
from jax.sharding import PartitionSpec as P

BLOCK = 64
PAIR = 2 * BLOCK
STEPS = 4
PAIRS = 8
ROWS = 16
COLS = 16
SLOTS = 2 * PAIRS + 4
SOLVE_ITERS = 7
SPECTRUM_TOP = 372.0
MESSAGE = 40
ORDER = (7, 0, 6, 1, 5, 2, 4, 3)
READY = {5: (6,), 2: (1,), 4: (5,), 3: (2, 3, 4)}
FAR_FIRST = (2, 1, 3)
FIRST_CUTS = (0, 32, 96, 128)
LATER_CUTS = (0, 24, 64)
MESH = pl.DeviceIdType.MESH


def dot(a, b, dims=((1,), (0,))):
    return lax.dot_general(a, b, (dims, ((), ())), preferred_element_type=jnp.float32)


def pieces(value, count):
    parts = []
    for index in range(count):
        part = value.astype(jnp.bfloat16)
        parts.append(part)
        if index < count - 1:
            value = value - part.astype(jnp.float32)
    return parts


def turn_pieces(turn):
    return jnp.concatenate([jnp.concatenate([part, part], axis=1) for part in pieces(turn, 3)], axis=0)


def turned(stacked, block):
    rows = stacked.shape[0] // 3
    out = dot(stacked, jnp.concatenate(pieces(block, 2), axis=0))
    return out[:rows] + (out[rows : 2 * rows] + out[2 * rows :])


def fine_product(left, right):
    out = dot(jnp.concatenate(pieces(left, 3), axis=0), jnp.concatenate(pieces(right, 3), axis=1))

    def term(i, j):
        return out[i * PAIR : (i + 1) * PAIR, j * PAIR : (j + 1) * PAIR]

    return term(0, 0) + ((term(0, 1) + term(1, 0)) + (term(1, 1) + (term(0, 2) + term(2, 0))))


def iota(axis):
    return lax.broadcasted_iota(jnp.int32, (PAIR, PAIR), axis)


def solve_turn(message):
    folded = message[:32]
    cross = jnp.concatenate([pltpu.roll(folded, BLOCK, 1), folded], axis=0)
    norms = message[32:33]
    bottom_norms = jnp.broadcast_to(norms, (BLOCK, PAIR))
    top_norms = jnp.transpose(jnp.broadcast_to(norms, (PAIR, PAIR)))[:BLOCK]
    spread = bottom_norms - top_norms
    square = spread * spread + 4.0 * cross * cross
    radius = jnp.sqrt(square)
    scale_term = (top_norms + bottom_norms) / BLOCK
    coupling = 2.0 * cross * spread / (square + jnp.abs(spread) * radius + scale_term * scale_term)
    lane = lax.broadcasted_iota(jnp.int32, (BLOCK, PAIR), 1)
    upper = jnp.where(lane >= BLOCK, coupling, 0.0)
    upper = jnp.concatenate([upper, jnp.zeros_like(upper)], axis=0)
    skew = upper - jnp.transpose(upper)
    identity = (iota(0) == iota(1)).astype(jnp.float32)

    def product(left, right):
        high, low = pieces(left, 2)
        tall = jnp.concatenate(
            [jnp.concatenate([high, high], axis=1), jnp.concatenate([low, low], axis=1)], axis=0
        )
        both = dot(tall, jnp.concatenate(pieces(right, 2), axis=0))
        return both[:PAIR] + both[PAIR:]

    alpha = 2.0 / (1.0 + SPECTRUM_TOP)
    delta = (SPECTRUM_TOP - 1.0) / (SPECTRUM_TOP + 1.0)
    left = (1.0 - alpha) * identity + alpha * product(skew, skew)
    result = alpha * (identity - skew)
    for step in range(SOLVE_ITERS):
        scale = 2.0 / (2.0 - delta * delta)
        delta = delta * delta / (2.0 - delta * delta)
        if step < SOLVE_ITERS - 1:
            both = product(left, jnp.concatenate([left, result], axis=1))
            result = scale * (result + both[:, PAIR:])
            left = (1.0 - scale) * identity + scale * both[:, :PAIR]
        else:
            result = result + product(left, result)
    rest = identity - result - fine_product(skew, result)
    result = result + fine_product(result, rest)
    return 2.0 * result - identity


def make_gram(both):
    top = jnp.concatenate(pieces(both[:BLOCK], 3), axis=0)
    bottom = jnp.concatenate(pieces(both[BLOCK:], 3), axis=0)
    out = dot(top, bottom, ((1,), (1,)))

    def term(i, j):
        return out[i * BLOCK : (i + 1) * BLOCK, j * BLOCK : (j + 1) * BLOCK]

    cross = term(0, 0) + ((term(0, 1) + term(1, 0)) + (term(1, 1) + (term(0, 2) + term(2, 0))))
    squares = both * both
    total = squares[:, :128]
    for piece in range(1, squares.shape[1] // 128):
        total = total + squares[:, piece * 128 : (piece + 1) * 128]
    norms = jnp.sum(jnp.transpose(total), axis=0, keepdims=True)
    return jnp.concatenate([cross[:32], cross[32:]], axis=1), jnp.broadcast_to(norms, (8, 128))


def sweep(order_ref, x_hbm, last_x, last_turns, last_edges, xin, buf, gram, gram_in, half_sum, half_in,
          turns, edges, in_sem, out_sem, gram_send, gram_recv, swap_send, swap_recv, turn_send, turn_recv, pass_send,
          edge_send, edge_recv, first_send, first_recv, halo_send, halo_recv):
    row = lax.axis_index("row")
    col = lax.axis_index("col")
    half = row // PAIRS
    mine = row % PAIRS
    core = row % 2
    partner = row + 1 - 2 * core
    opposite = (row + PAIRS) % ROWS
    has_left = col > 0
    has_right = col < COLS - 1
    at_first = col == 0
    at_last = col == COLS - 1

    load = pltpu.make_async_copy(x_hbm, xin, in_sem)
    load.start()

    barrier = pltpu.get_barrier_semaphore()
    for other in range(1, PAIRS):
        near = half * PAIRS + (mine + other) % PAIRS
        pl.semaphore_signal(barrier, inc=1, device_id={"row": near, "col": col}, device_id_type=MESH)
    pl.semaphore_signal(barrier, inc=1, device_id={"row": opposite, "col": col}, device_id_type=MESH)

    @pl.when(has_left)
    def _():
        pl.semaphore_signal(barrier, inc=1, device_id={"row": row, "col": col - 1}, device_id_type=MESH)

    @pl.when(has_right)
    def _():
        pl.semaphore_signal(barrier, inc=1, device_id={"row": row, "col": col + 1}, device_id_type=MESH)

    pl.semaphore_wait(barrier, PAIRS + has_left.astype(jnp.int32) + has_right.astype(jnp.int32))
    load.wait()

    def place(slot):
        source = order_ref[slot] & (2 * PAIRS - 1)
        buf[0, pl.ds(PAIR + slot * BLOCK, BLOCK), :] = xin[source]

    def remote(src, dst, send, recv, row_to, col_to):
        return pltpu.make_async_remote_copy(
            src_ref=src, dst_ref=dst, send_sem=send, recv_sem=recv,
            device_id={"row": row_to, "col": col_to}, device_id_type=MESH,
        )

    def first_right(cut):
        low, high = FIRST_CUTS[cut], FIRST_CUTS[cut + 1]
        return remote(buf.at[0, pl.ds(PAIRS * PAIR + low, high - low)], buf.at[0, pl.ds(low, high - low)],
                      first_send.at[0, cut], first_recv.at[0, cut], row, col + 1)

    def first_left(cut):
        low, high = FIRST_CUTS[cut], FIRST_CUTS[cut + 1]
        return remote(buf.at[0, pl.ds(PAIR + low, high - low)],
                      buf.at[0, pl.ds((PAIRS + 1) * PAIR + low, high - low)],
                      first_send.at[1, cut], first_recv.at[1, cut], row, col - 1)

    def halo_right(step, cut):
        low, high = LATER_CUTS[cut], LATER_CUTS[cut + 1]
        return remote(buf.at[step, pl.ds(16 * BLOCK + low, high - low)], buf.at[step, pl.ds(low, high - low)],
                      halo_send.at[step, cut], halo_recv.at[step, cut], row, col + 1)

    def halo_left(step, cut):
        low, high = LATER_CUTS[cut], LATER_CUTS[cut + 1]
        return remote(buf.at[step, pl.ds(3 * BLOCK + low, high - low)],
                      buf.at[step, pl.ds(19 * BLOCK + low, high - low)],
                      halo_send.at[step, 2 + cut], halo_recv.at[step, 2 + cut], row, col - 1)

    def edge_right(step):
        return remote(turns.at[step, PAIRS - 1, pl.ds(0, BLOCK)], edges.at[step, 0],
                      edge_send.at[step, 0], edge_recv.at[step, 0], row, col + 1)

    def edge_left(step):
        return remote(turns.at[step, 0, pl.ds(BLOCK, BLOCK)], edges.at[step, 1],
                      edge_send.at[step, 1], edge_recv.at[step, 1], row, col - 1)

    def gram_out(step, pair):
        return remote(gram.at[step, pair], gram_in.at[step, mine], gram_send.at[step, pair],
                      gram_recv.at[step, mine], half * PAIRS + pair, col)

    def gram_from(step, source):
        return remote(gram.at[step, mine], gram_in.at[step, source], gram_send.at[step, 0],
                      gram_recv.at[step, source], half * PAIRS + source, col)

    def swap(step):
        return remote(half_sum.at[step], half_in.at[step], swap_send.at[step], swap_recv.at[step], opposite, col)

    def turn_out(step, index):
        along = (mine + 2 * FAR_FIRST[index]) % PAIRS
        return remote(turns.at[step, mine], turns.at[step, mine], turn_send.at[step, index],
                      turn_recv.at[step, mine], half * PAIRS + along, col)

    def turn_pass(step, pair):
        return remote(turns.at[step, pair], turns.at[step, pair], pass_send.at[step, pair],
                      turn_recv.at[step, pair], partner, col)

    def send_gram(step, pair):
        folded, norms = make_gram(buf[step, pl.ds((pair + 1) * PAIR, PAIR), :])
        gram[step, pair, :32, :] = folded
        gram[step, pair, 32:, :] = norms

        @pl.when(mine != pair)
        def _():
            gram_out(step, pair).start()

    def sides(right, left):
        pl.when(has_right)(right)
        pl.when(has_left)(left)

    def solve_and_send(step):
        total = gram[step, mine]
        for other in range(1, PAIRS):
            source = (mine + other) % PAIRS
            gram_from(step, source).wait_recv()
            total = total + gram_in[step, source]
        half_sum[step] = total
        swap(step).start()

        @pl.when(step == 0)
        def _():
            sides(lambda: first_right(1).start(), lambda: first_left(1).start())

        @pl.when(step > 0)
        def _():
            sides(lambda: halo_right(step, 1).start(), lambda: halo_left(step, 1).start())

        swap(step).wait_recv()
        turns[step, mine] = solve_turn(total + half_in[step])
        for index in range(len(FAR_FIRST)):
            turn_out(step, index).start()
        turn_pass(step, mine).start()

    def send_edge(step, pair):
        if pair == PAIRS - 1:
            pl.when(has_right)(lambda: edge_right(step).start())
        if pair == 0:
            pl.when(has_left)(lambda: edge_left(step).start())

    def pass_turns(step):
        for pair in ORDER:
            @pl.when(core == pair % 2)
            def _():
                @pl.when(mine != pair)
                def _():
                    turn_pass(step, pair).wait_recv()
                    turn_pass(step, pair).start()
                send_edge(step, pair)

    def take_turn(step, pair):
        @pl.when(core != pair % 2)
        def _():
            turn_pass(step, pair).wait_recv()
            send_edge(step, pair)

    def rows_of(slot):
        return pl.ds(pl.multiple_of(slot * BLOCK, BLOCK), BLOCK)

    for slot in (14, 15, 0, 1):
        place(slot)
    sides(lambda: first_right(0).start(), lambda: first_left(0).start())
    for pair in (7, 0) + tuple(range(1, PAIRS - 1)):
        if pair not in (0, PAIRS - 1):
            place(2 * pair)
            place(2 * pair + 1)
        send_gram(0, pair)

    def one_step(step, carry):
        solve_and_send(step)
        pass_turns(step)
        for pair in (PAIRS - 1, 0):
            take_turn(step, pair)
        for pair in ORDER:
            if pair not in (0, PAIRS - 1):
                take_turn(step, pair)
            out = turned(turn_pieces(turns[step, pair]), buf[step, pl.ds((pair + 1) * PAIR, PAIR), :])
            top_slot, bottom_slot = 2 * pair + 4, 2 * pair + 1
            if pair == 0:
                top_slot = jnp.where(at_first, 2, top_slot)
                bottom_slot = jnp.where(at_first, 4, bottom_slot)
            if pair == PAIRS - 1:
                top_slot = jnp.where(at_last, 17, top_slot)
            buf[step + 1, rows_of(top_slot), :] = out[:BLOCK]
            buf[step + 1, rows_of(bottom_slot), :] = out[BLOCK:]
            for ready in READY.get(pair, ()):
                send_gram(step + 1, ready)

        @pl.when(step == 0)
        def _():
            sides(lambda: first_right(2).start(), lambda: first_left(2).start())

        sides(lambda: halo_right(step + 1, 0).start(), lambda: halo_left(step + 1, 0).start())

        @pl.when(has_left)
        def _():
            @pl.when(step == 0)
            def _():
                for cut in range(len(FIRST_CUTS) - 1):
                    first_right(cut).wait_recv()

            @pl.when(step > 0)
            def _():
                for cut in range(len(LATER_CUTS) - 1):
                    halo_right(step, cut).wait_recv()
            edge_right(step).wait_recv()
            buf[step + 1, pl.ds(2 * BLOCK, BLOCK), :] = turned(
                turn_pieces(edges[step, 0]), buf[step, pl.ds(0, PAIR), :]
            )

        send_gram(step + 1, 0)

        @pl.when(has_right)
        def _():
            @pl.when(step == 0)
            def _():
                for cut in range(len(FIRST_CUTS) - 1):
                    first_left(cut).wait_recv()

            @pl.when(step > 0)
            def _():
                for cut in range(len(LATER_CUTS) - 1):
                    halo_left(step, cut).wait_recv()
            edge_left(step).wait_recv()
            buf[step + 1, pl.ds(17 * BLOCK, BLOCK), :] = turned(
                turn_pieces(edges[step, 1]), buf[step, pl.ds((PAIRS + 1) * PAIR, PAIR), :]
            )

        send_gram(step + 1, PAIRS - 1)
        return carry

    lax.fori_loop(0, STEPS - 1, one_step, 0)

    last = STEPS - 1
    inner = pl.ds(BLOCK, (SLOTS - 2) * BLOCK)
    store_inner = pltpu.make_async_copy(buf.at[last, inner], last_x.at[inner], out_sem.at[0])
    store_inner.start()
    solve_and_send(last)
    pass_turns(last)
    for pair in ORDER:
        take_turn(last, pair)
    store_turns = pltpu.make_async_copy(turns.at[last], last_turns, out_sem.at[1])
    store_turns.start()

    def store_side(side):
        rows = pl.ds(side * (SLOTS - 1) * BLOCK, BLOCK)
        return (
            pltpu.make_async_copy(buf.at[last, rows], last_x.at[rows], out_sem.at[2 + side]),
            pltpu.make_async_copy(edges.at[last, side], last_edges.at[side], out_sem.at[4 + side]),
        )

    @pl.when(has_left)
    def _():
        for cut in range(len(LATER_CUTS) - 1):
            halo_right(last, cut).wait_recv()
        edge_right(last).wait_recv()
        for copy in store_side(0):
            copy.start()

    @pl.when(has_right)
    def _():
        for cut in range(len(LATER_CUTS) - 1):
            halo_left(last, cut).wait_recv()
        edge_left(last).wait_recv()
        for copy in store_side(1):
            copy.start()

    def drain(step, carry):
        for pair in range(PAIRS):
            @pl.when(mine != pair)
            def _():
                gram_out(step, pair).wait_send()

            @pl.when(core == pair % 2)
            def _():
                turn_pass(step, pair).wait_send()

        swap(step).wait_send()
        for index in range(len(FAR_FIRST)):
            turn_out(step, index).wait_send()

        sides(lambda: edge_right(step).wait_send(), lambda: edge_left(step).wait_send())

        @pl.when(step > 0)
        def _():
            for cut in range(len(LATER_CUTS) - 1):
                sides(lambda: halo_right(step, cut).wait_send(), lambda: halo_left(step, cut).wait_send())
        return carry

    lax.fori_loop(0, STEPS, drain, 0)
    for cut in range(len(FIRST_CUTS) - 1):
        sides(lambda: first_right(cut).wait_send(), lambda: first_left(cut).wait_send())
    store_inner.wait()
    store_turns.wait()

    @pl.when(has_left)
    def _():
        for copy in store_side(0):
            copy.wait()

    @pl.when(has_right)
    def _():
        for copy in store_side(1):
            copy.wait()


def finish(position, x_ref, turns_ref, edges_ref, out_ref):
    at_first = position[0] == 0
    at_last = position[0] == COLS - 1

    def put(slot, value):
        out_ref[slot * BLOCK : (slot + 1) * BLOCK, :] = value

    for pair in range(PAIRS):
        out = turned(turn_pieces(turns_ref[pair]), x_ref[(pair + 1) * PAIR : (pair + 2) * PAIR, :])
        top, bottom = out[:BLOCK], out[BLOCK:]
        if pair == 0:
            left = turned(turn_pieces(edges_ref[0]), x_ref[:PAIR, :])
            put(0, jnp.where(at_first, top, left))
            put(2, jnp.where(at_first, bottom, top))
        elif pair == PAIRS - 1:
            right = turned(turn_pieces(edges_ref[1]), x_ref[(PAIRS + 1) * PAIR :, :])
            put(2 * pair - 1, bottom)
            put(2 * pair + 1, jnp.where(at_last, top, right))
        else:
            put(2 * pair - 1, bottom)
            put(2 * pair + 2, top)


def local(columns, block_order):
    length = columns.shape[1]
    blocks = columns.reshape(2 * PAIRS, BLOCK, length)
    dma = pltpu.SemaphoreType.DMA
    position = lax.axis_index("col").astype(jnp.int32).reshape(1)
    last_x, last_turns, last_edges = pl.pallas_call(
        sweep,
        out_shape=(
            jax.ShapeDtypeStruct((SLOTS * BLOCK, length), jnp.float32),
            jax.ShapeDtypeStruct((PAIRS, PAIR, PAIR), jnp.float32),
            jax.ShapeDtypeStruct((2, BLOCK, PAIR), jnp.float32),
        ),
        in_specs=[
            pl.BlockSpec(memory_space=pltpu.SMEM),
            pl.BlockSpec(memory_space=pl.ANY),
        ],
        out_specs=(pl.BlockSpec(memory_space=pl.ANY),) * 3,
        scratch_shapes=[
            pltpu.VMEM(blocks.shape, jnp.float32),
            pltpu.VMEM((STEPS, SLOTS * BLOCK, length), jnp.float32),
            pltpu.VMEM((STEPS, PAIRS, MESSAGE, PAIR), jnp.float32),
            pltpu.VMEM((STEPS, PAIRS, MESSAGE, PAIR), jnp.float32),
            pltpu.VMEM((STEPS, MESSAGE, PAIR), jnp.float32),
            pltpu.VMEM((STEPS, MESSAGE, PAIR), jnp.float32),
            pltpu.VMEM((STEPS, PAIRS, PAIR, PAIR), jnp.float32),
            pltpu.VMEM((STEPS, 2, BLOCK, PAIR), jnp.float32),
            dma,
            dma((6,)),
            dma((STEPS, PAIRS)),
            dma((STEPS, PAIRS)),
            dma((STEPS,)),
            dma((STEPS,)),
            dma((STEPS, len(FAR_FIRST))),
            dma((STEPS, PAIRS)),
            dma((STEPS, PAIRS)),
            dma((STEPS, 2)),
            dma((STEPS, 2)),
            dma((2, len(FIRST_CUTS) - 1)),
            dma((2, len(FIRST_CUTS) - 1)),
            dma((STEPS, 2 * len(LATER_CUTS) - 2)),
            dma((STEPS, 2 * len(LATER_CUTS) - 2)),
        ],
        compiler_params=pltpu.CompilerParams(
            collective_id=0, has_side_effects=True, vmem_limit_bytes=58 * 1024 * 1024
        ),
    )(block_order, blocks)
    wide = 256
    return pl.pallas_call(
        finish,
        grid=(length // wide,),
        out_shape=jax.ShapeDtypeStruct(columns.shape, jnp.float32),
        in_specs=[
            pl.BlockSpec(memory_space=pltpu.SMEM),
            pl.BlockSpec((SLOTS * BLOCK, wide), lambda part: (0, part)),
            pl.BlockSpec((PAIRS, PAIR, PAIR), lambda part: (0, 0, 0)),
            pl.BlockSpec((2, BLOCK, PAIR), lambda part: (0, 0, 0)),
        ],
        out_specs=pl.BlockSpec((columns.shape[0], wide), lambda part: (0, part)),
    )(position, last_x, last_turns, last_edges)


def solution(mesh):
    placed = (P("col", "row"), P("col"))
    return jax.shard_map(
        local, mesh=mesh, in_specs=placed, out_specs=P("col", "row"), check_vma=False
    )
```

```python
import jax
import jax.numpy as jnp
from jax import lax
from jax.experimental import pallas as pl
from jax.experimental.pallas import tpu as pltpu
from jax.sharding import PartitionSpec as P

BLOCK = 64
PAIR = 2 * BLOCK
STEPS = 4
PAIRS = 8
ROWS = 16
COLS = 16
SLOTS = 2 * PAIRS + 4
SOLVE_ITERS = 7
SPECTRUM_TOP = 372.0
MESSAGE = 40
ORDER = (7, 0, 6, 1, 5, 2, 4, 3)
READY = {5: (6,), 2: (1,), 4: (5,), 3: (2, 3, 4)}
FAR_FIRST = (2, 1, 3)
FIRST_CUTS = (0, 48, 120, 128)
LATER_CUTS = (0, 8, 64)
MESH = pl.DeviceIdType.MESH


def dot(a, b, dims=((1,), (0,))):
    return lax.dot_general(a, b, (dims, ((), ())), preferred_element_type=jnp.float32)


def pieces(value, count):
    parts = []
    for index in range(count):
        part = value.astype(jnp.bfloat16)
        parts.append(part)
        if index < count - 1:
            value = value - part.astype(jnp.float32)
    return parts


def summed(left, right, terms):
    lefts = pieces(left, 1 + max(i for i, _ in terms))
    rights = pieces(right, 1 + max(j for _, j in terms))
    wide = jnp.concatenate([lefts[i] for i, _ in terms], axis=1)
    tall = jnp.concatenate([rights[j] for _, j in terms], axis=0)
    return dot(wide, tall)


ROUGH = ((0, 0), (0, 1), (1, 0), (1, 1))
TURN = ROUGH + ((2, 0), (2, 1))
FINE = ROUGH + ((0, 2), (2, 0))


def iota(axis):
    return lax.broadcasted_iota(jnp.int32, (PAIR, PAIR), axis)


def solve_turn(message):
    folded = message[:32]
    cross = jnp.concatenate([pltpu.roll(folded, BLOCK, 1), folded], axis=0)
    norms = message[32:33]
    bottom_norms = jnp.broadcast_to(norms, (BLOCK, PAIR))
    top_norms = jnp.transpose(jnp.broadcast_to(norms, (PAIR, PAIR)))[:BLOCK]
    spread = bottom_norms - top_norms
    square = spread * spread + 4.0 * cross * cross
    radius = jnp.sqrt(square)
    scale_term = (top_norms + bottom_norms) / BLOCK
    coupling = 2.0 * cross * spread / (square + jnp.abs(spread) * radius + scale_term * scale_term)
    lane = lax.broadcasted_iota(jnp.int32, (BLOCK, PAIR), 1)
    upper = jnp.where(lane >= BLOCK, coupling, 0.0)
    upper = jnp.concatenate([upper, jnp.zeros_like(upper)], axis=0)
    skew = upper - jnp.transpose(upper)
    identity = (iota(0) == iota(1)).astype(jnp.float32)

    alpha = 2.0 / (1.0 + SPECTRUM_TOP)
    delta = (SPECTRUM_TOP - 1.0) / (SPECTRUM_TOP + 1.0)
    left = (1.0 - alpha) * identity + alpha * summed(skew, skew, ROUGH)
    result = alpha * (identity - skew)
    for step in range(SOLVE_ITERS):
        scale = 2.0 / (2.0 - delta * delta)
        delta = delta * delta / (2.0 - delta * delta)
        if step < SOLVE_ITERS - 1:
            both = summed(left, jnp.concatenate([left, result], axis=1), ROUGH)
            result = scale * (result + both[:, PAIR:])
            left = (1.0 - scale) * identity + scale * both[:, :PAIR]
        else:
            result = result + summed(left, result, ROUGH)
    rest = identity - result - summed(skew, result, FINE)
    result = result + summed(result, rest, FINE)
    return 2.0 * result - identity


def make_gram(both):
    top = jnp.concatenate(pieces(both[:BLOCK], 2), axis=0)
    bottom = jnp.concatenate(pieces(both[BLOCK:], 2), axis=0)
    out = dot(top, bottom, ((1,), (1,)))

    def term(i, j):
        return out[i * BLOCK : (i + 1) * BLOCK, j * BLOCK : (j + 1) * BLOCK]

    cross = term(0, 0) + ((term(0, 1) + term(1, 0)) + term(1, 1))
    squares = both * both
    total = squares[:, :128]
    for piece in range(1, squares.shape[1] // 128):
        total = total + squares[:, piece * 128 : (piece + 1) * 128]
    norms = jnp.sum(jnp.transpose(total), axis=0, keepdims=True)
    return jnp.concatenate([cross[:32], cross[32:]], axis=1), jnp.broadcast_to(norms, (8, 128))


def sweep(order_ref, x_hbm, last_x, last_turns, last_edges, xin, buf, gram, gram_in, half_sum, half_in,
          turns, edges, in_sem, out_sem, gram_send, gram_recv, swap_send, swap_recv, turn_send, turn_recv, pass_send,
          edge_send, edge_recv, first_send, first_recv, halo_send, halo_recv):
    row = lax.axis_index("row")
    col = lax.axis_index("col")
    half = row // PAIRS
    mine = row % PAIRS
    core = row % 2
    partner = row + 1 - 2 * core
    opposite = (row + PAIRS) % ROWS
    has_left = col > 0
    has_right = col < COLS - 1
    at_first = col == 0
    at_last = col == COLS - 1

    load = pltpu.make_async_copy(x_hbm, xin, in_sem)
    load.start()

    barrier = pltpu.get_barrier_semaphore()
    for other in range(1, PAIRS):
        near = half * PAIRS + (mine + other) % PAIRS
        pl.semaphore_signal(barrier, inc=1, device_id={"row": near, "col": col}, device_id_type=MESH)
    pl.semaphore_signal(barrier, inc=1, device_id={"row": opposite, "col": col}, device_id_type=MESH)

    @pl.when(has_left)
    def _():
        pl.semaphore_signal(barrier, inc=1, device_id={"row": row, "col": col - 1}, device_id_type=MESH)

    @pl.when(has_right)
    def _():
        pl.semaphore_signal(barrier, inc=1, device_id={"row": row, "col": col + 1}, device_id_type=MESH)

    pl.semaphore_wait(barrier, PAIRS + has_left.astype(jnp.int32) + has_right.astype(jnp.int32))
    load.wait()

    def place(slot):
        source = order_ref[slot] & (2 * PAIRS - 1)
        buf[0, pl.ds(PAIR + slot * BLOCK, BLOCK), :] = xin[source]

    def remote(src, dst, send, recv, row_to, col_to):
        return pltpu.make_async_remote_copy(
            src_ref=src, dst_ref=dst, send_sem=send, recv_sem=recv,
            device_id={"row": row_to, "col": col_to}, device_id_type=MESH,
        )

    def first_right(cut):
        low, high = FIRST_CUTS[cut], FIRST_CUTS[cut + 1]
        return remote(buf.at[0, pl.ds(PAIRS * PAIR + low, high - low)], buf.at[0, pl.ds(low, high - low)],
                      first_send.at[0, cut], first_recv.at[0, cut], row, col + 1)

    def first_left(cut):
        low, high = FIRST_CUTS[cut], FIRST_CUTS[cut + 1]
        return remote(buf.at[0, pl.ds(PAIR + low, high - low)],
                      buf.at[0, pl.ds((PAIRS + 1) * PAIR + low, high - low)],
                      first_send.at[1, cut], first_recv.at[1, cut], row, col - 1)

    def halo_right(step, cut):
        low, high = LATER_CUTS[cut], LATER_CUTS[cut + 1]
        return remote(buf.at[step, pl.ds(16 * BLOCK + low, high - low)], buf.at[step, pl.ds(low, high - low)],
                      halo_send.at[step, cut], halo_recv.at[step, cut], row, col + 1)

    def halo_left(step, cut):
        low, high = LATER_CUTS[cut], LATER_CUTS[cut + 1]
        return remote(buf.at[step, pl.ds(3 * BLOCK + low, high - low)],
                      buf.at[step, pl.ds(19 * BLOCK + low, high - low)],
                      halo_send.at[step, 2 + cut], halo_recv.at[step, 2 + cut], row, col - 1)

    def edge_right(step):
        return remote(turns.at[step, PAIRS - 1, pl.ds(0, BLOCK)], edges.at[step, 0],
                      edge_send.at[step, 0], edge_recv.at[step, 0], row, col + 1)

    def edge_left(step):
        return remote(turns.at[step, 0, pl.ds(BLOCK, BLOCK)], edges.at[step, 1],
                      edge_send.at[step, 1], edge_recv.at[step, 1], row, col - 1)

    def gram_out(step, pair):
        return remote(gram.at[step, pair], gram_in.at[step, mine], gram_send.at[step, pair],
                      gram_recv.at[step, mine], half * PAIRS + pair, col)

    def gram_from(step, source):
        return remote(gram.at[step, mine], gram_in.at[step, source], gram_send.at[step, 0],
                      gram_recv.at[step, source], half * PAIRS + source, col)

    def swap(step):
        return remote(half_sum.at[step], half_in.at[step], swap_send.at[step], swap_recv.at[step], opposite, col)

    def turn_out(step, index):
        along = (mine + 2 * FAR_FIRST[index]) % PAIRS
        return remote(turns.at[step, mine], turns.at[step, mine], turn_send.at[step, index],
                      turn_recv.at[step, mine], half * PAIRS + along, col)

    def turn_pass(step, pair):
        return remote(turns.at[step, pair], turns.at[step, pair], pass_send.at[step, pair],
                      turn_recv.at[step, pair], partner, col)

    def send_gram(step, pair):
        folded, norms = make_gram(buf[step, pl.ds((pair + 1) * PAIR, PAIR), :])
        gram[step, pair, :32, :] = folded
        gram[step, pair, 32:, :] = norms

        @pl.when(mine != pair)
        def _():
            gram_out(step, pair).start()

    def sides(right, left):
        pl.when(has_right)(right)
        pl.when(has_left)(left)

    def solve_and_send(step):
        total = gram[step, mine]
        for other in range(1, PAIRS):
            source = (mine + other) % PAIRS
            gram_from(step, source).wait_recv()
            total = total + gram_in[step, source]
        half_sum[step] = total
        swap(step).start()

        @pl.when(step == 0)
        def _():
            sides(lambda: first_right(1).start(), lambda: first_left(1).start())

        @pl.when(step > 0)
        def _():
            sides(lambda: halo_right(step, 1).start(), lambda: halo_left(step, 1).start())

        swap(step).wait_recv()
        turns[step, mine] = solve_turn(total + half_in[step])
        for index in range(len(FAR_FIRST)):
            turn_out(step, index).start()
        turn_pass(step, mine).start()

    def send_edge(step, pair):
        if pair == PAIRS - 1:
            pl.when(has_right)(lambda: edge_right(step).start())
        if pair == 0:
            pl.when(has_left)(lambda: edge_left(step).start())

    def pass_turns(step):
        for pair in ORDER:
            @pl.when(core == pair % 2)
            def _():
                @pl.when(mine != pair)
                def _():
                    turn_pass(step, pair).wait_recv()
                    turn_pass(step, pair).start()
                send_edge(step, pair)

    def take_turn(step, pair):
        @pl.when(core != pair % 2)
        def _():
            turn_pass(step, pair).wait_recv()
            send_edge(step, pair)

    def rows_of(slot):
        return pl.ds(pl.multiple_of(slot * BLOCK, BLOCK), BLOCK)

    for slot in (14, 15, 0, 1):
        place(slot)
    sides(lambda: first_right(0).start(), lambda: first_left(0).start())
    for pair in (7, 0) + tuple(range(1, PAIRS - 1)):
        if pair not in (0, PAIRS - 1):
            place(2 * pair)
            place(2 * pair + 1)
        send_gram(0, pair)

    def one_step(step, carry):
        solve_and_send(step)
        pass_turns(step)
        for pair in (PAIRS - 1, 0):
            take_turn(step, pair)
        for pair in ORDER:
            if pair not in (0, PAIRS - 1):
                take_turn(step, pair)
            out = summed(turns[step, pair], buf[step, pl.ds((pair + 1) * PAIR, PAIR), :], TURN)
            top_slot, bottom_slot = 2 * pair + 4, 2 * pair + 1
            if pair == 0:
                top_slot = jnp.where(at_first, 2, top_slot)
                bottom_slot = jnp.where(at_first, 4, bottom_slot)
            if pair == PAIRS - 1:
                top_slot = jnp.where(at_last, 17, top_slot)
            buf[step + 1, rows_of(top_slot), :] = out[:BLOCK]
            buf[step + 1, rows_of(bottom_slot), :] = out[BLOCK:]
            for ready in READY.get(pair, ()):
                send_gram(step + 1, ready)

        @pl.when(step == 0)
        def _():
            sides(lambda: first_right(2).start(), lambda: first_left(2).start())

        sides(lambda: halo_right(step + 1, 0).start(), lambda: halo_left(step + 1, 0).start())

        @pl.when(has_left)
        def _():
            @pl.when(step == 0)
            def _():
                for cut in range(len(FIRST_CUTS) - 1):
                    first_right(cut).wait_recv()

            @pl.when(step > 0)
            def _():
                for cut in range(len(LATER_CUTS) - 1):
                    halo_right(step, cut).wait_recv()
            edge_right(step).wait_recv()
            buf[step + 1, pl.ds(2 * BLOCK, BLOCK), :] = summed(
                edges[step, 0], buf[step, pl.ds(0, PAIR), :], TURN
            )

        send_gram(step + 1, 0)

        @pl.when(has_right)
        def _():
            @pl.when(step == 0)
            def _():
                for cut in range(len(FIRST_CUTS) - 1):
                    first_left(cut).wait_recv()

            @pl.when(step > 0)
            def _():
                for cut in range(len(LATER_CUTS) - 1):
                    halo_left(step, cut).wait_recv()
            edge_left(step).wait_recv()
            buf[step + 1, pl.ds(17 * BLOCK, BLOCK), :] = summed(
                edges[step, 1], buf[step, pl.ds((PAIRS + 1) * PAIR, PAIR), :], TURN
            )

        send_gram(step + 1, PAIRS - 1)
        return carry

    lax.fori_loop(0, STEPS - 1, one_step, 0)

    last = STEPS - 1
    inner = pl.ds(BLOCK, (SLOTS - 2) * BLOCK)
    store_inner = pltpu.make_async_copy(buf.at[last, inner], last_x.at[inner], out_sem.at[0])
    store_inner.start()
    solve_and_send(last)
    pass_turns(last)
    for pair in ORDER:
        take_turn(last, pair)
    store_turns = pltpu.make_async_copy(turns.at[last], last_turns, out_sem.at[1])
    store_turns.start()

    def store_side(side):
        rows = pl.ds(side * (SLOTS - 1) * BLOCK, BLOCK)
        return (
            pltpu.make_async_copy(buf.at[last, rows], last_x.at[rows], out_sem.at[2 + side]),
            pltpu.make_async_copy(edges.at[last, side], last_edges.at[side], out_sem.at[4 + side]),
        )

    @pl.when(has_left)
    def _():
        for cut in range(len(LATER_CUTS) - 1):
            halo_right(last, cut).wait_recv()
        edge_right(last).wait_recv()
        for copy in store_side(0):
            copy.start()

    @pl.when(has_right)
    def _():
        for cut in range(len(LATER_CUTS) - 1):
            halo_left(last, cut).wait_recv()
        edge_left(last).wait_recv()
        for copy in store_side(1):
            copy.start()

    def drain(step, carry):
        for pair in range(PAIRS):
            @pl.when(mine != pair)
            def _():
                gram_out(step, pair).wait_send()

            @pl.when(core == pair % 2)
            def _():
                turn_pass(step, pair).wait_send()

        swap(step).wait_send()
        for index in range(len(FAR_FIRST)):
            turn_out(step, index).wait_send()

        sides(lambda: edge_right(step).wait_send(), lambda: edge_left(step).wait_send())

        @pl.when(step > 0)
        def _():
            for cut in range(len(LATER_CUTS) - 1):
                sides(lambda: halo_right(step, cut).wait_send(), lambda: halo_left(step, cut).wait_send())
        return carry

    lax.fori_loop(0, STEPS, drain, 0)
    for cut in range(len(FIRST_CUTS) - 1):
        sides(lambda: first_right(cut).wait_send(), lambda: first_left(cut).wait_send())
    store_inner.wait()
    store_turns.wait()

    @pl.when(has_left)
    def _():
        for copy in store_side(0):
            copy.wait()

    @pl.when(has_right)
    def _():
        for copy in store_side(1):
            copy.wait()


def finish(position, x_ref, turns_ref, edges_ref, out_ref):
    at_first = position[0] == 0
    at_last = position[0] == COLS - 1

    def put(slot, value):
        out_ref[slot * BLOCK : (slot + 1) * BLOCK, :] = value

    for pair in range(PAIRS):
        out = summed(turns_ref[pair], x_ref[(pair + 1) * PAIR : (pair + 2) * PAIR, :], ROUGH)
        top, bottom = out[:BLOCK], out[BLOCK:]
        if pair == 0:
            left = summed(edges_ref[0], x_ref[:PAIR, :], ROUGH)
            put(0, jnp.where(at_first, top, left))
            put(2, jnp.where(at_first, bottom, top))
        elif pair == PAIRS - 1:
            right = summed(edges_ref[1], x_ref[(PAIRS + 1) * PAIR :, :], ROUGH)
            put(2 * pair - 1, bottom)
            put(2 * pair + 1, jnp.where(at_last, top, right))
        else:
            put(2 * pair - 1, bottom)
            put(2 * pair + 2, top)


def local(columns, block_order):
    length = columns.shape[1]
    blocks = columns.reshape(2 * PAIRS, BLOCK, length)
    dma = pltpu.SemaphoreType.DMA
    position = lax.axis_index("col").astype(jnp.int32).reshape(1)
    last_x, last_turns, last_edges = pl.pallas_call(
        sweep,
        out_shape=(
            jax.ShapeDtypeStruct((SLOTS * BLOCK, length), jnp.float32),
            jax.ShapeDtypeStruct((PAIRS, PAIR, PAIR), jnp.float32),
            jax.ShapeDtypeStruct((2, BLOCK, PAIR), jnp.float32),
        ),
        in_specs=[
            pl.BlockSpec(memory_space=pltpu.SMEM),
            pl.BlockSpec(memory_space=pl.ANY),
        ],
        out_specs=(pl.BlockSpec(memory_space=pl.ANY),) * 3,
        scratch_shapes=[
            pltpu.VMEM(blocks.shape, jnp.float32),
            pltpu.VMEM((STEPS, SLOTS * BLOCK, length), jnp.float32),
            pltpu.VMEM((STEPS, PAIRS, MESSAGE, PAIR), jnp.float32),
            pltpu.VMEM((STEPS, PAIRS, MESSAGE, PAIR), jnp.float32),
            pltpu.VMEM((STEPS, MESSAGE, PAIR), jnp.float32),
            pltpu.VMEM((STEPS, MESSAGE, PAIR), jnp.float32),
            pltpu.VMEM((STEPS, PAIRS, PAIR, PAIR), jnp.float32),
            pltpu.VMEM((STEPS, 2, BLOCK, PAIR), jnp.float32),
            dma,
            dma((6,)),
            dma((STEPS, PAIRS)),
            dma((STEPS, PAIRS)),
            dma((STEPS,)),
            dma((STEPS,)),
            dma((STEPS, len(FAR_FIRST))),
            dma((STEPS, PAIRS)),
            dma((STEPS, PAIRS)),
            dma((STEPS, 2)),
            dma((STEPS, 2)),
            dma((2, len(FIRST_CUTS) - 1)),
            dma((2, len(FIRST_CUTS) - 1)),
            dma((STEPS, 2 * len(LATER_CUTS) - 2)),
            dma((STEPS, 2 * len(LATER_CUTS) - 2)),
        ],
        compiler_params=pltpu.CompilerParams(
            collective_id=0, has_side_effects=True, vmem_limit_bytes=58 * 1024 * 1024
        ),
    )(block_order, blocks)
    wide = 256
    return pl.pallas_call(
        finish,
        grid=(length // wide,),
        out_shape=jax.ShapeDtypeStruct(columns.shape, jnp.float32),
        in_specs=[
            pl.BlockSpec(memory_space=pltpu.SMEM),
            pl.BlockSpec((SLOTS * BLOCK, wide), lambda part: (0, part)),
            pl.BlockSpec((PAIRS, PAIR, PAIR), lambda part: (0, 0, 0)),
            pl.BlockSpec((2, BLOCK, PAIR), lambda part: (0, 0, 0)),
        ],
        out_specs=pl.BlockSpec((columns.shape[0], wide), lambda part: (0, part)),
    )(position, last_x, last_turns, last_edges)


def solution(mesh):
    placed = (P("col", "row"), P("col"))
    return jax.shard_map(
        local, mesh=mesh, in_specs=placed, out_specs=P("col", "row"), check_vma=False
    )
```

```python
import jax
import jax.numpy as jnp
from jax import lax
from jax.experimental import pallas as pl
from jax.experimental.pallas import tpu as pltpu
from jax.sharding import PartitionSpec as P

BLOCK = 64
PAIR = 2 * BLOCK
STEPS = 4
PAIRS = 8
ROWS = 16
COLS = 16
SLOTS = 2 * PAIRS + 4
SOLVE_ITERS = 7
SPECTRUM_TOP = 372.0
MESSAGE = 40
ORDER = (7, 0, 6, 1, 5, 2, 4, 3)
READY = {2: ((6, 1),), 3: ((5, 2), (4, 3))}
FAR_FIRST = (2, 1, 3)
FIRST_CUTS = (0, 48, 120, 128)
LATER_CUTS = (0, 8, 64)
MESH = pl.DeviceIdType.MESH


def dot(a, b, dims=((1,), (0,))):
    return lax.dot_general(a, b, (dims, ((), ())), preferred_element_type=jnp.float32)


def pieces(value, count):
    parts = []
    for index in range(count):
        part = value.astype(jnp.bfloat16)
        parts.append(part)
        if index < count - 1:
            value = value - part.astype(jnp.float32)
    return parts


def summed(left, right, terms):
    lefts = pieces(left, 1 + max(i for i, _ in terms))
    rights = pieces(right, 1 + max(j for _, j in terms))
    wide = jnp.concatenate([lefts[i] for i, _ in terms], axis=1)
    tall = jnp.concatenate([rights[j] for _, j in terms], axis=0)
    return dot(wide, tall)


ROUGH = ((0, 0), (0, 1), (1, 0), (1, 1))
TURN = ROUGH + ((2, 0), (2, 1))
FINE = ROUGH + ((0, 2), (2, 0))


def iota(axis):
    return lax.broadcasted_iota(jnp.int32, (PAIR, PAIR), axis)


def solve_turn(message):
    folded = message[:32]
    cross = jnp.concatenate([pltpu.roll(folded, BLOCK, 1), folded], axis=0)
    norms = message[32:33]
    bottom_norms = jnp.broadcast_to(norms, (BLOCK, PAIR))
    top_norms = jnp.transpose(jnp.broadcast_to(norms, (PAIR, PAIR)))[:BLOCK]
    spread = bottom_norms - top_norms
    square = spread * spread + 4.0 * cross * cross
    radius = jnp.sqrt(square)
    scale_term = (top_norms + bottom_norms) / BLOCK
    coupling = 2.0 * cross * spread / (square + jnp.abs(spread) * radius + scale_term * scale_term)
    lane = lax.broadcasted_iota(jnp.int32, (BLOCK, PAIR), 1)
    upper = jnp.where(lane >= BLOCK, coupling, 0.0)
    upper = jnp.concatenate([upper, jnp.zeros_like(upper)], axis=0)
    skew = upper - jnp.transpose(upper)
    identity = (iota(0) == iota(1)).astype(jnp.float32)

    alpha = 2.0 / (1.0 + SPECTRUM_TOP)
    delta = (SPECTRUM_TOP - 1.0) / (SPECTRUM_TOP + 1.0)
    left = (1.0 - alpha) * identity + alpha * summed(skew, skew, ROUGH)
    result = alpha * (identity - skew)
    for step in range(SOLVE_ITERS):
        scale = 2.0 / (2.0 - delta * delta)
        delta = delta * delta / (2.0 - delta * delta)
        if step < SOLVE_ITERS - 1:
            both = summed(left, jnp.concatenate([left, result], axis=1), ROUGH)
            result = scale * (result + both[:, PAIR:])
            left = (1.0 - scale) * identity + scale * both[:, :PAIR]
        else:
            result = result + summed(left, result, ROUGH)
    rest = identity - result - summed(skew, result, FINE)
    result = result + summed(result, rest, FINE)
    return 2.0 * result - identity


def make_grams(first, second):
    def stacked(start):
        rows = slice(start, start + BLOCK)
        return jnp.concatenate(pieces(first[rows], 2) + pieces(second[rows], 2), axis=0)

    out = dot(stacked(0), stacked(BLOCK), ((1,), (1,)))
    results = []
    for index, both in enumerate((first, second)):
        whole = out[index * PAIR : (index + 1) * PAIR, index * PAIR : (index + 1) * PAIR]
        whole = whole[:BLOCK] + whole[BLOCK:]
        cross = whole + pltpu.roll(whole, BLOCK, 1)
        lane = lax.broadcasted_iota(jnp.int32, (32, PAIR), 1)
        folded = jnp.where(lane < BLOCK, cross[:32], cross[32:])
        squares = both * both
        total = squares[:, :128]
        for piece in range(1, squares.shape[1] // 128):
            total = total + squares[:, piece * 128 : (piece + 1) * 128]
        norms = jnp.sum(jnp.transpose(total), axis=0, keepdims=True)
        results.append((folded, jnp.broadcast_to(norms, (8, 128))))
    return results


def sweep(order_ref, x_hbm, last_x, last_turns, last_edges, xin, buf, gram, gram_in, half_sum, half_in,
          turns, edges, in_sem, out_sem, gram_send, gram_recv, swap_send, swap_recv, turn_send, turn_recv, pass_send,
          edge_send, edge_recv, first_send, first_recv, halo_send, halo_recv):
    row = lax.axis_index("row")
    col = lax.axis_index("col")
    half = row // PAIRS
    mine = row % PAIRS
    core = row % 2
    partner = row + 1 - 2 * core
    opposite = (row + PAIRS) % ROWS
    has_left = col > 0
    has_right = col < COLS - 1
    at_first = col == 0
    at_last = col == COLS - 1

    load = pltpu.make_async_copy(x_hbm, xin, in_sem)
    load.start()

    barrier = pltpu.get_barrier_semaphore()
    for other in range(1, PAIRS):
        near = half * PAIRS + (mine + other) % PAIRS
        pl.semaphore_signal(barrier, inc=1, device_id={"row": near, "col": col}, device_id_type=MESH)
    pl.semaphore_signal(barrier, inc=1, device_id={"row": opposite, "col": col}, device_id_type=MESH)

    @pl.when(has_left)
    def _():
        pl.semaphore_signal(barrier, inc=1, device_id={"row": row, "col": col - 1}, device_id_type=MESH)

    @pl.when(has_right)
    def _():
        pl.semaphore_signal(barrier, inc=1, device_id={"row": row, "col": col + 1}, device_id_type=MESH)

    pl.semaphore_wait(barrier, PAIRS + has_left.astype(jnp.int32) + has_right.astype(jnp.int32))
    load.wait()

    def place(slot):
        source = order_ref[slot] & (2 * PAIRS - 1)
        buf[0, pl.ds(PAIR + slot * BLOCK, BLOCK), :] = xin[source]

    def remote(src, dst, send, recv, row_to, col_to):
        return pltpu.make_async_remote_copy(
            src_ref=src, dst_ref=dst, send_sem=send, recv_sem=recv,
            device_id={"row": row_to, "col": col_to}, device_id_type=MESH,
        )

    def first_right(cut):
        low, high = FIRST_CUTS[cut], FIRST_CUTS[cut + 1]
        return remote(buf.at[0, pl.ds(PAIRS * PAIR + low, high - low)], buf.at[0, pl.ds(low, high - low)],
                      first_send.at[0, cut], first_recv.at[0, cut], row, col + 1)

    def first_left(cut):
        low, high = FIRST_CUTS[cut], FIRST_CUTS[cut + 1]
        return remote(buf.at[0, pl.ds(PAIR + low, high - low)],
                      buf.at[0, pl.ds((PAIRS + 1) * PAIR + low, high - low)],
                      first_send.at[1, cut], first_recv.at[1, cut], row, col - 1)

    def halo_right(step, cut):
        low, high = LATER_CUTS[cut], LATER_CUTS[cut + 1]
        return remote(buf.at[step, pl.ds(16 * BLOCK + low, high - low)], buf.at[step, pl.ds(low, high - low)],
                      halo_send.at[step, cut], halo_recv.at[step, cut], row, col + 1)

    def halo_left(step, cut):
        low, high = LATER_CUTS[cut], LATER_CUTS[cut + 1]
        return remote(buf.at[step, pl.ds(3 * BLOCK + low, high - low)],
                      buf.at[step, pl.ds(19 * BLOCK + low, high - low)],
                      halo_send.at[step, 2 + cut], halo_recv.at[step, 2 + cut], row, col - 1)

    def edge_right(step):
        return remote(turns.at[step, PAIRS - 1, pl.ds(0, BLOCK)], edges.at[step, 0],
                      edge_send.at[step, 0], edge_recv.at[step, 0], row, col + 1)

    def edge_left(step):
        return remote(turns.at[step, 0, pl.ds(BLOCK, BLOCK)], edges.at[step, 1],
                      edge_send.at[step, 1], edge_recv.at[step, 1], row, col - 1)

    def gram_out(step, pair):
        return remote(gram.at[step, pair], gram_in.at[step, mine], gram_send.at[step, pair],
                      gram_recv.at[step, mine], half * PAIRS + pair, col)

    def gram_from(step, source):
        return remote(gram.at[step, mine], gram_in.at[step, source], gram_send.at[step, 0],
                      gram_recv.at[step, source], half * PAIRS + source, col)

    def swap(step):
        return remote(half_sum.at[step], half_in.at[step], swap_send.at[step], swap_recv.at[step], opposite, col)

    def turn_out(step, index):
        along = (mine + 2 * FAR_FIRST[index]) % PAIRS
        return remote(turns.at[step, mine], turns.at[step, mine], turn_send.at[step, index],
                      turn_recv.at[step, mine], half * PAIRS + along, col)

    def turn_pass(step, pair):
        return remote(turns.at[step, pair], turns.at[step, pair], pass_send.at[step, pair],
                      turn_recv.at[step, pair], partner, col)

    def send_grams(step, couple):
        loaded = [buf[step, pl.ds((pair + 1) * PAIR, PAIR), :] for pair in couple]
        for pair, (folded, norms) in zip(couple, make_grams(*loaded)):
            gram[step, pair, :32, :] = folded
            gram[step, pair, 32:, :] = norms
        for pair in couple:
            @pl.when(mine != pair)
            def _():
                gram_out(step, pair).start()

    def sides(right, left):
        pl.when(has_right)(right)
        pl.when(has_left)(left)

    def solve_and_send(step):
        total = gram[step, mine]
        for other in range(1, PAIRS):
            source = (mine + other) % PAIRS
            gram_from(step, source).wait_recv()
            total = total + gram_in[step, source]
        half_sum[step] = total
        swap(step).start()

        @pl.when(step == 0)
        def _():
            sides(lambda: first_right(1).start(), lambda: first_left(1).start())

        @pl.when(step > 0)
        def _():
            sides(lambda: halo_right(step, 1).start(), lambda: halo_left(step, 1).start())

        swap(step).wait_recv()
        turns[step, mine] = solve_turn(total + half_in[step])
        for index in range(len(FAR_FIRST)):
            turn_out(step, index).start()
        turn_pass(step, mine).start()

    def send_edge(step, pair):
        if pair == PAIRS - 1:
            pl.when(has_right)(lambda: edge_right(step).start())
        if pair == 0:
            pl.when(has_left)(lambda: edge_left(step).start())

    def pass_turns(step):
        for pair in ORDER:
            @pl.when(core == pair % 2)
            def _():
                @pl.when(mine != pair)
                def _():
                    turn_pass(step, pair).wait_recv()
                    turn_pass(step, pair).start()
                send_edge(step, pair)

    def take_turn(step, pair):
        @pl.when(core != pair % 2)
        def _():
            turn_pass(step, pair).wait_recv()
            send_edge(step, pair)

    def rows_of(slot):
        return pl.ds(pl.multiple_of(slot * BLOCK, BLOCK), BLOCK)

    for slot in (14, 15, 0, 1):
        place(slot)
    sides(lambda: first_right(0).start(), lambda: first_left(0).start())
    for couple in ((7, 0), (6, 1), (5, 2), (4, 3)):
        for pair in couple:
            if pair not in (0, PAIRS - 1):
                place(2 * pair)
                place(2 * pair + 1)
        send_grams(0, couple)

    def one_step(step, carry):
        solve_and_send(step)
        pass_turns(step)
        for pair in ORDER:
            take_turn(step, pair)
        for pair in ORDER:
            out = summed(turns[step, pair], buf[step, pl.ds((pair + 1) * PAIR, PAIR), :], TURN)
            top_slot, bottom_slot = 2 * pair + 4, 2 * pair + 1
            if pair == 0:
                top_slot = jnp.where(at_first, 2, top_slot)
                bottom_slot = jnp.where(at_first, 4, bottom_slot)
            if pair == PAIRS - 1:
                top_slot = jnp.where(at_last, 17, top_slot)
            buf[step + 1, rows_of(top_slot), :] = out[:BLOCK]
            buf[step + 1, rows_of(bottom_slot), :] = out[BLOCK:]
            for ready in READY.get(pair, ()):
                send_grams(step + 1, ready)

        @pl.when(step == 0)
        def _():
            sides(lambda: first_right(2).start(), lambda: first_left(2).start())

        sides(lambda: halo_right(step + 1, 0).start(), lambda: halo_left(step + 1, 0).start())

        @pl.when(has_left)
        def _():
            @pl.when(step == 0)
            def _():
                for cut in range(len(FIRST_CUTS) - 1):
                    first_right(cut).wait_recv()

            @pl.when(step > 0)
            def _():
                for cut in range(len(LATER_CUTS) - 1):
                    halo_right(step, cut).wait_recv()
            edge_right(step).wait_recv()
            buf[step + 1, pl.ds(2 * BLOCK, BLOCK), :] = summed(
                edges[step, 0], buf[step, pl.ds(0, PAIR), :], TURN
            )

        @pl.when(has_right)
        def _():
            @pl.when(step == 0)
            def _():
                for cut in range(len(FIRST_CUTS) - 1):
                    first_left(cut).wait_recv()

            @pl.when(step > 0)
            def _():
                for cut in range(len(LATER_CUTS) - 1):
                    halo_left(step, cut).wait_recv()
            edge_left(step).wait_recv()
            buf[step + 1, pl.ds(17 * BLOCK, BLOCK), :] = summed(
                edges[step, 1], buf[step, pl.ds((PAIRS + 1) * PAIR, PAIR), :], TURN
            )

        send_grams(step + 1, (PAIRS - 1, 0))
        return carry

    lax.fori_loop(0, STEPS - 1, one_step, 0)

    last = STEPS - 1
    inner = pl.ds(BLOCK, (SLOTS - 2) * BLOCK)
    store_inner = pltpu.make_async_copy(buf.at[last, inner], last_x.at[inner], out_sem.at[0])
    store_inner.start()
    solve_and_send(last)
    pass_turns(last)
    for pair in ORDER:
        take_turn(last, pair)
    store_turns = pltpu.make_async_copy(turns.at[last], last_turns, out_sem.at[1])
    store_turns.start()

    def store_side(side):
        rows = pl.ds(side * (SLOTS - 1) * BLOCK, BLOCK)
        return (
            pltpu.make_async_copy(buf.at[last, rows], last_x.at[rows], out_sem.at[2 + side]),
            pltpu.make_async_copy(edges.at[last, side], last_edges.at[side], out_sem.at[4 + side]),
        )

    @pl.when(has_left)
    def _():
        for cut in range(len(LATER_CUTS) - 1):
            halo_right(last, cut).wait_recv()
        edge_right(last).wait_recv()
        for copy in store_side(0):
            copy.start()

    @pl.when(has_right)
    def _():
        for cut in range(len(LATER_CUTS) - 1):
            halo_left(last, cut).wait_recv()
        edge_left(last).wait_recv()
        for copy in store_side(1):
            copy.start()

    def drain(step, carry):
        for pair in range(PAIRS):
            @pl.when(mine != pair)
            def _():
                gram_out(step, pair).wait_send()

            @pl.when(core == pair % 2)
            def _():
                turn_pass(step, pair).wait_send()

        swap(step).wait_send()
        for index in range(len(FAR_FIRST)):
            turn_out(step, index).wait_send()

        sides(lambda: edge_right(step).wait_send(), lambda: edge_left(step).wait_send())

        @pl.when(step > 0)
        def _():
            for cut in range(len(LATER_CUTS) - 1):
                sides(lambda: halo_right(step, cut).wait_send(), lambda: halo_left(step, cut).wait_send())
        return carry

    lax.fori_loop(0, STEPS, drain, 0)
    for cut in range(len(FIRST_CUTS) - 1):
        sides(lambda: first_right(cut).wait_send(), lambda: first_left(cut).wait_send())
    store_inner.wait()
    store_turns.wait()

    @pl.when(has_left)
    def _():
        for copy in store_side(0):
            copy.wait()

    @pl.when(has_right)
    def _():
        for copy in store_side(1):
            copy.wait()


def finish(position, x_ref, turns_ref, edges_ref, out_ref):
    at_first = position[0] == 0
    at_last = position[0] == COLS - 1

    def put(slot, value):
        out_ref[slot * BLOCK : (slot + 1) * BLOCK, :] = value

    for pair in range(PAIRS):
        out = summed(turns_ref[pair], x_ref[(pair + 1) * PAIR : (pair + 2) * PAIR, :], ROUGH)
        top, bottom = out[:BLOCK], out[BLOCK:]
        if pair == 0:
            left = summed(edges_ref[0], x_ref[:PAIR, :], ROUGH)
            put(0, jnp.where(at_first, top, left))
            put(2, jnp.where(at_first, bottom, top))
        elif pair == PAIRS - 1:
            right = summed(edges_ref[1], x_ref[(PAIRS + 1) * PAIR :, :], ROUGH)
            put(2 * pair - 1, bottom)
            put(2 * pair + 1, jnp.where(at_last, top, right))
        else:
            put(2 * pair - 1, bottom)
            put(2 * pair + 2, top)


def local(columns, block_order):
    length = columns.shape[1]
    blocks = columns.reshape(2 * PAIRS, BLOCK, length)
    dma = pltpu.SemaphoreType.DMA
    position = lax.axis_index("col").astype(jnp.int32).reshape(1)
    last_x, last_turns, last_edges = pl.pallas_call(
        sweep,
        out_shape=(
            jax.ShapeDtypeStruct((SLOTS * BLOCK, length), jnp.float32),
            jax.ShapeDtypeStruct((PAIRS, PAIR, PAIR), jnp.float32),
            jax.ShapeDtypeStruct((2, BLOCK, PAIR), jnp.float32),
        ),
        in_specs=[
            pl.BlockSpec(memory_space=pltpu.SMEM),
            pl.BlockSpec(memory_space=pl.ANY),
        ],
        out_specs=(pl.BlockSpec(memory_space=pl.ANY),) * 3,
        scratch_shapes=[
            pltpu.VMEM(blocks.shape, jnp.float32),
            pltpu.VMEM((STEPS, SLOTS * BLOCK, length), jnp.float32),
            pltpu.VMEM((STEPS, PAIRS, MESSAGE, PAIR), jnp.float32),
            pltpu.VMEM((STEPS, PAIRS, MESSAGE, PAIR), jnp.float32),
            pltpu.VMEM((STEPS, MESSAGE, PAIR), jnp.float32),
            pltpu.VMEM((STEPS, MESSAGE, PAIR), jnp.float32),
            pltpu.VMEM((STEPS, PAIRS, PAIR, PAIR), jnp.float32),
            pltpu.VMEM((STEPS, 2, BLOCK, PAIR), jnp.float32),
            dma,
            dma((6,)),
            dma((STEPS, PAIRS)),
            dma((STEPS, PAIRS)),
            dma((STEPS,)),
            dma((STEPS,)),
            dma((STEPS, len(FAR_FIRST))),
            dma((STEPS, PAIRS)),
            dma((STEPS, PAIRS)),
            dma((STEPS, 2)),
            dma((STEPS, 2)),
            dma((2, len(FIRST_CUTS) - 1)),
            dma((2, len(FIRST_CUTS) - 1)),
            dma((STEPS, 2 * len(LATER_CUTS) - 2)),
            dma((STEPS, 2 * len(LATER_CUTS) - 2)),
        ],
        compiler_params=pltpu.CompilerParams(
            collective_id=0, has_side_effects=True, vmem_limit_bytes=58 * 1024 * 1024
        ),
    )(block_order, blocks)
    wide = 256
    return pl.pallas_call(
        finish,
        grid=(length // wide,),
        out_shape=jax.ShapeDtypeStruct(columns.shape, jnp.float32),
        in_specs=[
            pl.BlockSpec(memory_space=pltpu.SMEM),
            pl.BlockSpec((SLOTS * BLOCK, wide), lambda part: (0, part)),
            pl.BlockSpec((PAIRS, PAIR, PAIR), lambda part: (0, 0, 0)),
            pl.BlockSpec((2, BLOCK, PAIR), lambda part: (0, 0, 0)),
        ],
        out_specs=pl.BlockSpec((columns.shape[0], wide), lambda part: (0, part)),
    )(position, last_x, last_turns, last_edges)


def solution(mesh):
    placed = (P("col", "row"), P("col"))
    return jax.shard_map(
        local, mesh=mesh, in_specs=placed, out_specs=P("col", "row"), check_vma=False
    )
```

```python
import jax
import jax.numpy as jnp
from jax import lax
from jax.experimental import pallas as pl
from jax.experimental.pallas import tpu as pltpu
from jax.sharding import PartitionSpec as P

BLOCK = 64
PAIR = 2 * BLOCK
STEPS = 4
PAIRS = 8
ROWS = 16
COLS = 16
SLOTS = 2 * PAIRS + 4
SOLVE_ITERS = 7
SPECTRUM_TOP = 372.0
MESSAGE = 40
ORDER = (7, 0, 6, 1, 5, 2, 4, 3)
READY = {2: ((6, 1),), 3: ((5, 2),)}
FAR_FIRST = (2, 1, 3)
FIRST_CUTS = (0, 48, 120, 128)
LATER_CUTS = (0, 8, 64)
MESH = pl.DeviceIdType.MESH


def dot(a, b, dims=((1,), (0,))):
    return lax.dot_general(a, b, (dims, ((), ())), preferred_element_type=jnp.float32)


def pieces(value, count):
    parts = []
    for index in range(count):
        part = value.astype(jnp.bfloat16)
        parts.append(part)
        if index < count - 1:
            value = value - part.astype(jnp.float32)
    return parts


def summed(left, right, terms):
    lefts = pieces(left, 1 + max(i for i, _ in terms))
    rights = pieces(right, 1 + max(j for _, j in terms))
    wide = jnp.concatenate([lefts[i] for i, _ in terms], axis=1)
    tall = jnp.concatenate([rights[j] for _, j in terms], axis=0)
    return dot(wide, tall)


ROUGH = ((0, 0), (0, 1), (1, 0), (1, 1))
TURN = ROUGH + ((2, 0), (2, 1))
FINE = ROUGH + ((0, 2), (2, 0))


def iota(axis):
    return lax.broadcasted_iota(jnp.int32, (PAIR, PAIR), axis)


def solve_turn(message):
    folded = message[:32]
    cross = jnp.concatenate([pltpu.roll(folded, BLOCK, 1), folded], axis=0)
    norms = message[32:33]
    bottom_norms = jnp.broadcast_to(norms, (BLOCK, PAIR))
    top_norms = jnp.transpose(jnp.broadcast_to(norms, (PAIR, PAIR)))[:BLOCK]
    spread = bottom_norms - top_norms
    square = spread * spread + 4.0 * cross * cross
    radius = jnp.sqrt(square)
    scale_term = (top_norms + bottom_norms) / BLOCK
    coupling = 2.0 * cross * spread / (square + jnp.abs(spread) * radius + scale_term * scale_term)
    lane = lax.broadcasted_iota(jnp.int32, (BLOCK, PAIR), 1)
    upper = jnp.where(lane >= BLOCK, coupling, 0.0)
    upper = jnp.concatenate([upper, jnp.zeros_like(upper)], axis=0)
    skew = upper - jnp.transpose(upper)
    identity = (iota(0) == iota(1)).astype(jnp.float32)

    alpha = 2.0 / (1.0 + SPECTRUM_TOP)
    delta = (SPECTRUM_TOP - 1.0) / (SPECTRUM_TOP + 1.0)
    left = (1.0 - alpha) * identity + alpha * summed(skew, skew, ROUGH)
    result = alpha * (identity - skew)
    for step in range(SOLVE_ITERS):
        scale = 2.0 / (2.0 - delta * delta)
        delta = delta * delta / (2.0 - delta * delta)
        if step < SOLVE_ITERS - 1:
            both = summed(left, jnp.concatenate([left, result], axis=1), ROUGH)
            result = scale * (result + both[:, PAIR:])
            left = (1.0 - scale) * identity + scale * both[:, :PAIR]
        else:
            result = result + summed(left, result, ROUGH)
    rest = identity - result - summed(skew, result, FINE)
    result = result + summed(result, rest, FINE)
    return 2.0 * result - identity


def make_grams(first, second):
    def stacked(start):
        rows = slice(start, start + BLOCK)
        return jnp.concatenate(pieces(first[rows], 2) + pieces(second[rows], 2), axis=0)

    out = dot(stacked(0), stacked(BLOCK), ((1,), (1,)))
    results = []
    for index, both in enumerate((first, second)):
        whole = out[index * PAIR : (index + 1) * PAIR, index * PAIR : (index + 1) * PAIR]
        whole = whole[:BLOCK] + whole[BLOCK:]
        cross = whole + pltpu.roll(whole, BLOCK, 1)
        lane = lax.broadcasted_iota(jnp.int32, (32, PAIR), 1)
        folded = jnp.where(lane < BLOCK, cross[:32], cross[32:])
        squares = both * both
        total = squares[:, :128]
        for piece in range(1, squares.shape[1] // 128):
            total = total + squares[:, piece * 128 : (piece + 1) * 128]
        norms = jnp.sum(jnp.transpose(total), axis=0, keepdims=True)
        results.append((folded, jnp.broadcast_to(norms, (8, 128))))
    return results


def sweep(order_ref, x_hbm, last_x, last_turns, last_edges, xin, buf, gram, gram_in, half_sum, half_in,
          turns, edges, in_sem, out_sem, gram_send, gram_recv, swap_send, swap_recv, turn_send, turn_recv, pass_send,
          edge_send, edge_recv, first_send, first_recv, halo_send, halo_recv):
    row = lax.axis_index("row")
    col = lax.axis_index("col")
    half = row // PAIRS
    mine = row % PAIRS
    core = row % 2
    partner = row + 1 - 2 * core
    opposite = (row + PAIRS) % ROWS
    has_left = col > 0
    has_right = col < COLS - 1
    at_first = col == 0
    at_last = col == COLS - 1

    load = pltpu.make_async_copy(x_hbm, xin, in_sem)
    load.start()

    barrier = pltpu.get_barrier_semaphore()
    for other in range(1, PAIRS):
        near = half * PAIRS + (mine + other) % PAIRS
        pl.semaphore_signal(barrier, inc=1, device_id={"row": near, "col": col}, device_id_type=MESH)
    pl.semaphore_signal(barrier, inc=1, device_id={"row": opposite, "col": col}, device_id_type=MESH)

    @pl.when(has_left)
    def _():
        pl.semaphore_signal(barrier, inc=1, device_id={"row": row, "col": col - 1}, device_id_type=MESH)

    @pl.when(has_right)
    def _():
        pl.semaphore_signal(barrier, inc=1, device_id={"row": row, "col": col + 1}, device_id_type=MESH)

    pl.semaphore_wait(barrier, PAIRS + has_left.astype(jnp.int32) + has_right.astype(jnp.int32))
    load.wait()

    def place(slot):
        source = order_ref[slot] & (2 * PAIRS - 1)
        buf[0, pl.ds(PAIR + slot * BLOCK, BLOCK), :] = xin[source]

    def remote(src, dst, send, recv, row_to, col_to):
        return pltpu.make_async_remote_copy(
            src_ref=src, dst_ref=dst, send_sem=send, recv_sem=recv,
            device_id={"row": row_to, "col": col_to}, device_id_type=MESH,
        )

    def first_right(cut):
        low, high = FIRST_CUTS[cut], FIRST_CUTS[cut + 1]
        return remote(buf.at[0, pl.ds(PAIRS * PAIR + low, high - low)], buf.at[0, pl.ds(low, high - low)],
                      first_send.at[0, cut], first_recv.at[0, cut], row, col + 1)

    def first_left(cut):
        low, high = FIRST_CUTS[cut], FIRST_CUTS[cut + 1]
        return remote(buf.at[0, pl.ds(PAIR + low, high - low)],
                      buf.at[0, pl.ds((PAIRS + 1) * PAIR + low, high - low)],
                      first_send.at[1, cut], first_recv.at[1, cut], row, col - 1)

    def halo_right(step, cut):
        low, high = LATER_CUTS[cut], LATER_CUTS[cut + 1]
        return remote(buf.at[step, pl.ds(16 * BLOCK + low, high - low)], buf.at[step, pl.ds(low, high - low)],
                      halo_send.at[step, cut], halo_recv.at[step, cut], row, col + 1)

    def halo_left(step, cut):
        low, high = LATER_CUTS[cut], LATER_CUTS[cut + 1]
        return remote(buf.at[step, pl.ds(3 * BLOCK + low, high - low)],
                      buf.at[step, pl.ds(19 * BLOCK + low, high - low)],
                      halo_send.at[step, 2 + cut], halo_recv.at[step, 2 + cut], row, col - 1)

    def edge_right(step):
        return remote(turns.at[step, PAIRS - 1, pl.ds(0, BLOCK)], edges.at[step, 0],
                      edge_send.at[step, 0], edge_recv.at[step, 0], row, col + 1)

    def edge_left(step):
        return remote(turns.at[step, 0, pl.ds(BLOCK, BLOCK)], edges.at[step, 1],
                      edge_send.at[step, 1], edge_recv.at[step, 1], row, col - 1)

    def gram_out(step, pair):
        return remote(gram.at[step, pair], gram_in.at[step, mine], gram_send.at[step, pair],
                      gram_recv.at[step, mine], half * PAIRS + pair, col)

    def gram_from(step, source):
        return remote(gram.at[step, mine], gram_in.at[step, source], gram_send.at[step, 0],
                      gram_recv.at[step, source], half * PAIRS + source, col)

    def swap(step):
        return remote(half_sum.at[step], half_in.at[step], swap_send.at[step], swap_recv.at[step], opposite, col)

    def turn_out(step, index):
        along = (mine + 2 * FAR_FIRST[index]) % PAIRS
        return remote(turns.at[step, mine], turns.at[step, mine], turn_send.at[step, index],
                      turn_recv.at[step, mine], half * PAIRS + along, col)

    def turn_pass(step, pair):
        return remote(turns.at[step, pair], turns.at[step, pair], pass_send.at[step, pair],
                      turn_recv.at[step, pair], partner, col)

    def send_grams(step, couple):
        loaded = [buf[step, pl.ds((pair + 1) * PAIR, PAIR), :] for pair in couple]
        for pair, (folded, norms) in zip(couple, make_grams(*loaded)):
            gram[step, pair, :32, :] = folded
            gram[step, pair, 32:, :] = norms
        for pair in couple:
            @pl.when(mine != pair)
            def _():
                gram_out(step, pair).start()

    def sides(right, left):
        pl.when(has_right)(right)
        pl.when(has_left)(left)

    def solve_and_send(step):
        total = gram[step, mine]
        for other in range(1, PAIRS):
            source = (mine + other) % PAIRS
            gram_from(step, source).wait_recv()
            total = total + gram_in[step, source]
        half_sum[step] = total
        swap(step).start()

        @pl.when(step == 0)
        def _():
            sides(lambda: first_right(1).start(), lambda: first_left(1).start())

        @pl.when(step > 0)
        def _():
            sides(lambda: halo_right(step, 1).start(), lambda: halo_left(step, 1).start())

        swap(step).wait_recv()
        turns[step, mine] = solve_turn(total + half_in[step])
        for index in range(len(FAR_FIRST)):
            turn_out(step, index).start()
        turn_pass(step, mine).start()

    def send_edge(step, pair):
        if pair == PAIRS - 1:
            pl.when(has_right)(lambda: edge_right(step).start())
        if pair == 0:
            pl.when(has_left)(lambda: edge_left(step).start())

    def pass_turns(step):
        for pair in ORDER:
            @pl.when(core == pair % 2)
            def _():
                @pl.when(mine != pair)
                def _():
                    turn_pass(step, pair).wait_recv()
                    turn_pass(step, pair).start()
                send_edge(step, pair)

    def take_turn(step, pair):
        @pl.when(core != pair % 2)
        def _():
            turn_pass(step, pair).wait_recv()
            send_edge(step, pair)

    def rows_of(slot):
        return pl.ds(pl.multiple_of(slot * BLOCK, BLOCK), BLOCK)

    for slot in (14, 15, 0, 1):
        place(slot)
    sides(lambda: first_right(0).start(), lambda: first_left(0).start())
    for couple in ((7, 0), (6, 1), (5, 2), (4, 3)):
        for pair in couple:
            if pair not in (0, PAIRS - 1):
                place(2 * pair)
                place(2 * pair + 1)
        send_grams(0, couple)

    def one_step(step, carry):
        solve_and_send(step)
        pass_turns(step)
        for pair in ORDER:
            take_turn(step, pair)
        for pair in ORDER:
            out = summed(turns[step, pair], buf[step, pl.ds((pair + 1) * PAIR, PAIR), :], TURN)
            top_slot, bottom_slot = 2 * pair + 4, 2 * pair + 1
            if pair == 0:
                top_slot = jnp.where(at_first, 2, top_slot)
                bottom_slot = jnp.where(at_first, 4, bottom_slot)
            if pair == PAIRS - 1:
                top_slot = jnp.where(at_last, 17, top_slot)
            buf[step + 1, rows_of(top_slot), :] = out[:BLOCK]
            buf[step + 1, rows_of(bottom_slot), :] = out[BLOCK:]
            for ready in READY.get(pair, ()):
                send_grams(step + 1, ready)

        @pl.when(step == 0)
        def _():
            sides(lambda: first_right(2).start(), lambda: first_left(2).start())

        sides(lambda: halo_right(step + 1, 0).start(), lambda: halo_left(step + 1, 0).start())

        @pl.when(has_left)
        def _():
            @pl.when(step == 0)
            def _():
                for cut in range(len(FIRST_CUTS) - 1):
                    first_right(cut).wait_recv()

            @pl.when(step > 0)
            def _():
                for cut in range(len(LATER_CUTS) - 1):
                    halo_right(step, cut).wait_recv()
            edge_right(step).wait_recv()
            buf[step + 1, pl.ds(2 * BLOCK, BLOCK), :] = summed(
                edges[step, 0], buf[step, pl.ds(0, PAIR), :], TURN
            )

        @pl.when(has_right)
        def _():
            @pl.when(step == 0)
            def _():
                for cut in range(len(FIRST_CUTS) - 1):
                    first_left(cut).wait_recv()

            @pl.when(step > 0)
            def _():
                for cut in range(len(LATER_CUTS) - 1):
                    halo_left(step, cut).wait_recv()
            edge_left(step).wait_recv()
            buf[step + 1, pl.ds(17 * BLOCK, BLOCK), :] = summed(
                edges[step, 1], buf[step, pl.ds((PAIRS + 1) * PAIR, PAIR), :], TURN
            )

        send_grams(step + 1, (PAIRS - 1, 0))
        send_grams(step + 1, (4, 3))
        return carry

    lax.fori_loop(0, STEPS - 1, one_step, 0)

    last = STEPS - 1
    inner = pl.ds(BLOCK, (SLOTS - 2) * BLOCK)
    store_inner = pltpu.make_async_copy(buf.at[last, inner], last_x.at[inner], out_sem.at[0])
    store_inner.start()
    solve_and_send(last)
    pass_turns(last)
    for pair in ORDER:
        take_turn(last, pair)
    store_turns = pltpu.make_async_copy(turns.at[last], last_turns, out_sem.at[1])
    store_turns.start()

    def store_side(side):
        rows = pl.ds(side * (SLOTS - 1) * BLOCK, BLOCK)
        return (
            pltpu.make_async_copy(buf.at[last, rows], last_x.at[rows], out_sem.at[2 + side]),
            pltpu.make_async_copy(edges.at[last, side], last_edges.at[side], out_sem.at[4 + side]),
        )

    @pl.when(has_left)
    def _():
        for cut in range(len(LATER_CUTS) - 1):
            halo_right(last, cut).wait_recv()
        edge_right(last).wait_recv()
        for copy in store_side(0):
            copy.start()

    @pl.when(has_right)
    def _():
        for cut in range(len(LATER_CUTS) - 1):
            halo_left(last, cut).wait_recv()
        edge_left(last).wait_recv()
        for copy in store_side(1):
            copy.start()

    def drain(step, carry):
        for pair in range(PAIRS):
            @pl.when(mine != pair)
            def _():
                gram_out(step, pair).wait_send()

            @pl.when(core == pair % 2)
            def _():
                turn_pass(step, pair).wait_send()

        swap(step).wait_send()
        for index in range(len(FAR_FIRST)):
            turn_out(step, index).wait_send()

        sides(lambda: edge_right(step).wait_send(), lambda: edge_left(step).wait_send())

        @pl.when(step > 0)
        def _():
            for cut in range(len(LATER_CUTS) - 1):
                sides(lambda: halo_right(step, cut).wait_send(), lambda: halo_left(step, cut).wait_send())
        return carry

    lax.fori_loop(0, STEPS, drain, 0)
    for cut in range(len(FIRST_CUTS) - 1):
        sides(lambda: first_right(cut).wait_send(), lambda: first_left(cut).wait_send())
    store_inner.wait()
    store_turns.wait()

    @pl.when(has_left)
    def _():
        for copy in store_side(0):
            copy.wait()

    @pl.when(has_right)
    def _():
        for copy in store_side(1):
            copy.wait()


def finish(position, x_ref, turns_ref, edges_ref, out_ref):
    at_first = position[0] == 0
    at_last = position[0] == COLS - 1

    def put(slot, value):
        out_ref[slot * BLOCK : (slot + 1) * BLOCK, :] = value

    for pair in range(PAIRS):
        out = summed(turns_ref[pair], x_ref[(pair + 1) * PAIR : (pair + 2) * PAIR, :], ROUGH)
        top, bottom = out[:BLOCK], out[BLOCK:]
        if pair == 0:
            left = summed(edges_ref[0], x_ref[:PAIR, :], ROUGH)
            put(0, jnp.where(at_first, top, left))
            put(2, jnp.where(at_first, bottom, top))
        elif pair == PAIRS - 1:
            right = summed(edges_ref[1], x_ref[(PAIRS + 1) * PAIR :, :], ROUGH)
            put(2 * pair - 1, bottom)
            put(2 * pair + 1, jnp.where(at_last, top, right))
        else:
            put(2 * pair - 1, bottom)
            put(2 * pair + 2, top)


def local(columns, block_order):
    length = columns.shape[1]
    blocks = columns.reshape(2 * PAIRS, BLOCK, length)
    dma = pltpu.SemaphoreType.DMA
    position = lax.axis_index("col").astype(jnp.int32).reshape(1)
    last_x, last_turns, last_edges = pl.pallas_call(
        sweep,
        out_shape=(
            jax.ShapeDtypeStruct((SLOTS * BLOCK, length), jnp.float32),
            jax.ShapeDtypeStruct((PAIRS, PAIR, PAIR), jnp.float32),
            jax.ShapeDtypeStruct((2, BLOCK, PAIR), jnp.float32),
        ),
        in_specs=[
            pl.BlockSpec(memory_space=pltpu.SMEM),
            pl.BlockSpec(memory_space=pl.ANY),
        ],
        out_specs=(pl.BlockSpec(memory_space=pl.ANY),) * 3,
        scratch_shapes=[
            pltpu.VMEM(blocks.shape, jnp.float32),
            pltpu.VMEM((STEPS, SLOTS * BLOCK, length), jnp.float32),
            pltpu.VMEM((STEPS, PAIRS, MESSAGE, PAIR), jnp.float32),
            pltpu.VMEM((STEPS, PAIRS, MESSAGE, PAIR), jnp.float32),
            pltpu.VMEM((STEPS, MESSAGE, PAIR), jnp.float32),
            pltpu.VMEM((STEPS, MESSAGE, PAIR), jnp.float32),
            pltpu.VMEM((STEPS, PAIRS, PAIR, PAIR), jnp.float32),
            pltpu.VMEM((STEPS, 2, BLOCK, PAIR), jnp.float32),
            dma,
            dma((6,)),
            dma((STEPS, PAIRS)),
            dma((STEPS, PAIRS)),
            dma((STEPS,)),
            dma((STEPS,)),
            dma((STEPS, len(FAR_FIRST))),
            dma((STEPS, PAIRS)),
            dma((STEPS, PAIRS)),
            dma((STEPS, 2)),
            dma((STEPS, 2)),
            dma((2, len(FIRST_CUTS) - 1)),
            dma((2, len(FIRST_CUTS) - 1)),
            dma((STEPS, 2 * len(LATER_CUTS) - 2)),
            dma((STEPS, 2 * len(LATER_CUTS) - 2)),
        ],
        compiler_params=pltpu.CompilerParams(
            collective_id=0, has_side_effects=True, vmem_limit_bytes=58 * 1024 * 1024
        ),
    )(block_order, blocks)
    wide = 512
    return pl.pallas_call(
        finish,
        grid=(length // wide,),
        out_shape=jax.ShapeDtypeStruct(columns.shape, jnp.float32),
        in_specs=[
            pl.BlockSpec(memory_space=pltpu.SMEM),
            pl.BlockSpec((SLOTS * BLOCK, wide), lambda part: (0, part)),
            pl.BlockSpec((PAIRS, PAIR, PAIR), lambda part: (0, 0, 0)),
            pl.BlockSpec((2, BLOCK, PAIR), lambda part: (0, 0, 0)),
        ],
        out_specs=pl.BlockSpec((columns.shape[0], wide), lambda part: (0, part)),
    )(position, last_x, last_turns, last_edges)


def solution(mesh):
    placed = (P("col", "row"), P("col"))
    return jax.shard_map(
        local, mesh=mesh, in_specs=placed, out_specs=P("col", "row"), check_vma=False
    )
```

```python
import jax
import jax.numpy as jnp
from jax import lax
from jax.experimental import pallas as pl
from jax.experimental.pallas import tpu as pltpu
from jax.sharding import PartitionSpec as P

BLOCK = 64
PAIR = 2 * BLOCK
STEPS = 4
PAIRS = 8
ROWS = 16
COLS = 16
SLOTS = 2 * PAIRS + 4
SOLVE_ITERS = 7
SPECTRUM_TOP = 372.0
MESSAGE = 40
ORDER = (7, 0, 6, 1, 5, 2, 4, 3)
READY = {2: ((6, 1),)}
FAR_FIRST = (2, 1, 3)
FIRST_CUTS = (0, 48, 120, 128)
LATER_CUTS = (0, 8, 64)
MESH = pl.DeviceIdType.MESH


def dot(a, b, dims=((1,), (0,))):
    return lax.dot_general(a, b, (dims, ((), ())), preferred_element_type=jnp.float32)


def pieces(value, count):
    parts = []
    for index in range(count):
        part = value.astype(jnp.bfloat16)
        parts.append(part)
        if index < count - 1:
            value = value - part.astype(jnp.float32)
    return parts


def summed(left, right, terms):
    lefts = pieces(left, 1 + max(i for i, _ in terms))
    rights = pieces(right, 1 + max(j for _, j in terms))
    wide = jnp.concatenate([lefts[i] for i, _ in terms], axis=1)
    tall = jnp.concatenate([rights[j] for _, j in terms], axis=0)
    return dot(wide, tall)


ROUGH = ((0, 0), (0, 1), (1, 0), (1, 1))
TURN = ROUGH + ((2, 0), (2, 1))
FINE = ROUGH + ((0, 2), (2, 0))


def iota(axis):
    return lax.broadcasted_iota(jnp.int32, (PAIR, PAIR), axis)


def solve_turn(message):
    folded = message[:32]
    cross = jnp.concatenate([pltpu.roll(folded, BLOCK, 1), folded], axis=0)
    norms = message[32:33]
    bottom_norms = jnp.broadcast_to(norms, (BLOCK, PAIR))
    top_norms = jnp.transpose(jnp.broadcast_to(norms, (PAIR, PAIR)))[:BLOCK]
    spread = bottom_norms - top_norms
    square = spread * spread + 4.0 * cross * cross
    radius = jnp.sqrt(square)
    scale_term = (top_norms + bottom_norms) / BLOCK
    coupling = 2.0 * cross * spread / (square + jnp.abs(spread) * radius + scale_term * scale_term)
    lane = lax.broadcasted_iota(jnp.int32, (BLOCK, PAIR), 1)
    upper = jnp.where(lane >= BLOCK, coupling, 0.0)
    upper = jnp.concatenate([upper, jnp.zeros_like(upper)], axis=0)
    skew = upper - jnp.transpose(upper)
    identity = (iota(0) == iota(1)).astype(jnp.float32)

    alpha = 2.0 / (1.0 + SPECTRUM_TOP)
    delta = (SPECTRUM_TOP - 1.0) / (SPECTRUM_TOP + 1.0)
    left = (1.0 - alpha) * identity + alpha * summed(skew, skew, ROUGH)
    result = alpha * (identity - skew)
    for step in range(SOLVE_ITERS):
        scale = 2.0 / (2.0 - delta * delta)
        delta = delta * delta / (2.0 - delta * delta)
        if step < SOLVE_ITERS - 1:
            both = summed(left, jnp.concatenate([left, result], axis=1), ROUGH)
            result = scale * (result + both[:, PAIR:])
            left = (1.0 - scale) * identity + scale * both[:, :PAIR]
        else:
            result = result + summed(left, result, ROUGH)
    rest = identity - result - summed(skew, result, FINE)
    result = result + summed(result, rest, FINE)
    return 2.0 * result - identity


def make_grams(first, second):
    def stacked(start):
        rows = slice(start, start + BLOCK)
        return jnp.concatenate(pieces(first[rows], 2) + pieces(second[rows], 2), axis=0)

    out = dot(stacked(0), stacked(BLOCK), ((1,), (1,)))
    results = []
    for index, both in enumerate((first, second)):
        whole = out[index * PAIR : (index + 1) * PAIR, index * PAIR : (index + 1) * PAIR]
        whole = whole[:BLOCK] + whole[BLOCK:]
        cross = whole + pltpu.roll(whole, BLOCK, 1)
        lane = lax.broadcasted_iota(jnp.int32, (32, PAIR), 1)
        folded = jnp.where(lane < BLOCK, cross[:32], cross[32:])
        squares = both * both
        total = squares[:, :128]
        for piece in range(1, squares.shape[1] // 128):
            total = total + squares[:, piece * 128 : (piece + 1) * 128]
        norms = jnp.sum(jnp.transpose(total), axis=0, keepdims=True)
        results.append((folded, jnp.broadcast_to(norms, (8, 128))))
    return results


def sweep(order_ref, x_hbm, last_x, last_turns, last_edges, xin, buf, gram, gram_in, half_sum, half_in,
          turns, edges, in_sem, out_sem, gram_send, gram_recv, swap_send, swap_recv, turn_send, turn_recv, pass_send,
          edge_send, edge_recv, first_send, first_recv, halo_send, halo_recv):
    row = lax.axis_index("row")
    col = lax.axis_index("col")
    half = row // PAIRS
    mine = row % PAIRS
    core = row % 2
    partner = row + 1 - 2 * core
    opposite = (row + PAIRS) % ROWS
    has_left = col > 0
    has_right = col < COLS - 1
    at_first = col == 0
    at_last = col == COLS - 1

    load = pltpu.make_async_copy(x_hbm, xin, in_sem)
    load.start()

    barrier = pltpu.get_barrier_semaphore()
    for other in range(1, PAIRS):
        near = half * PAIRS + (mine + other) % PAIRS
        pl.semaphore_signal(barrier, inc=1, device_id={"row": near, "col": col}, device_id_type=MESH)
    pl.semaphore_signal(barrier, inc=1, device_id={"row": opposite, "col": col}, device_id_type=MESH)

    @pl.when(has_left)
    def _():
        pl.semaphore_signal(barrier, inc=1, device_id={"row": row, "col": col - 1}, device_id_type=MESH)

    @pl.when(has_right)
    def _():
        pl.semaphore_signal(barrier, inc=1, device_id={"row": row, "col": col + 1}, device_id_type=MESH)

    pl.semaphore_wait(barrier, PAIRS + has_left.astype(jnp.int32) + has_right.astype(jnp.int32))
    load.wait()

    def place(slot):
        source = order_ref[slot] & (2 * PAIRS - 1)
        buf[0, pl.ds(PAIR + slot * BLOCK, BLOCK), :] = xin[source]

    def remote(src, dst, send, recv, row_to, col_to):
        return pltpu.make_async_remote_copy(
            src_ref=src, dst_ref=dst, send_sem=send, recv_sem=recv,
            device_id={"row": row_to, "col": col_to}, device_id_type=MESH,
        )

    def first_right(cut):
        low, high = FIRST_CUTS[cut], FIRST_CUTS[cut + 1]
        return remote(buf.at[0, pl.ds(PAIRS * PAIR + low, high - low)], buf.at[0, pl.ds(low, high - low)],
                      first_send.at[0, cut], first_recv.at[0, cut], row, col + 1)

    def first_left(cut):
        low, high = FIRST_CUTS[cut], FIRST_CUTS[cut + 1]
        return remote(buf.at[0, pl.ds(PAIR + low, high - low)],
                      buf.at[0, pl.ds((PAIRS + 1) * PAIR + low, high - low)],
                      first_send.at[1, cut], first_recv.at[1, cut], row, col - 1)

    def halo_right(step, cut):
        low, high = LATER_CUTS[cut], LATER_CUTS[cut + 1]
        return remote(buf.at[step, pl.ds(16 * BLOCK + low, high - low)], buf.at[step, pl.ds(low, high - low)],
                      halo_send.at[step, cut], halo_recv.at[step, cut], row, col + 1)

    def halo_left(step, cut):
        low, high = LATER_CUTS[cut], LATER_CUTS[cut + 1]
        return remote(buf.at[step, pl.ds(3 * BLOCK + low, high - low)],
                      buf.at[step, pl.ds(19 * BLOCK + low, high - low)],
                      halo_send.at[step, 2 + cut], halo_recv.at[step, 2 + cut], row, col - 1)

    def edge_right(step):
        return remote(turns.at[step, PAIRS - 1, pl.ds(0, BLOCK)], edges.at[step, 0],
                      edge_send.at[step, 0], edge_recv.at[step, 0], row, col + 1)

    def edge_left(step):
        return remote(turns.at[step, 0, pl.ds(BLOCK, BLOCK)], edges.at[step, 1],
                      edge_send.at[step, 1], edge_recv.at[step, 1], row, col - 1)

    def gram_out(step, pair):
        return remote(gram.at[step, pair], gram_in.at[step, mine], gram_send.at[step, pair],
                      gram_recv.at[step, mine], half * PAIRS + pair, col)

    def gram_from(step, source):
        return remote(gram.at[step, mine], gram_in.at[step, source], gram_send.at[step, 0],
                      gram_recv.at[step, source], half * PAIRS + source, col)

    def swap(step):
        return remote(half_sum.at[step], half_in.at[step], swap_send.at[step], swap_recv.at[step], opposite, col)

    def turn_out(step, index):
        along = (mine + 2 * FAR_FIRST[index]) % PAIRS
        return remote(turns.at[step, mine], turns.at[step, mine], turn_send.at[step, index],
                      turn_recv.at[step, mine], half * PAIRS + along, col)

    def turn_pass(step, pair):
        return remote(turns.at[step, pair], turns.at[step, pair], pass_send.at[step, pair],
                      turn_recv.at[step, pair], partner, col)

    def send_grams(step, couple):
        loaded = [buf[step, pl.ds((pair + 1) * PAIR, PAIR), :] for pair in couple]
        for pair, (folded, norms) in zip(couple, make_grams(*loaded)):
            gram[step, pair, :32, :] = folded
            gram[step, pair, 32:, :] = norms
        for pair in couple:
            @pl.when(mine != pair)
            def _():
                gram_out(step, pair).start()

    def sides(right, left):
        pl.when(has_right)(right)
        pl.when(has_left)(left)

    def solve_and_send(step):
        total = gram[step, mine]
        for other in range(1, PAIRS):
            source = (mine + other) % PAIRS
            gram_from(step, source).wait_recv()
            total = total + gram_in[step, source]
        half_sum[step] = total
        swap(step).start()

        @pl.when(step == 0)
        def _():
            sides(lambda: first_right(1).start(), lambda: first_left(1).start())

        @pl.when(step > 0)
        def _():
            sides(lambda: halo_right(step, 1).start(), lambda: halo_left(step, 1).start())

        swap(step).wait_recv()
        turns[step, mine] = solve_turn(total + half_in[step])
        for index in range(len(FAR_FIRST)):
            turn_out(step, index).start()
        turn_pass(step, mine).start()

    def send_edge(step, pair):
        if pair == PAIRS - 1:
            pl.when(has_right)(lambda: edge_right(step).start())
        if pair == 0:
            pl.when(has_left)(lambda: edge_left(step).start())

    def pass_turns(step):
        for pair in ORDER:
            @pl.when(core == pair % 2)
            def _():
                @pl.when(mine != pair)
                def _():
                    turn_pass(step, pair).wait_recv()
                    turn_pass(step, pair).start()
                send_edge(step, pair)

    def take_turn(step, pair):
        @pl.when(core != pair % 2)
        def _():
            turn_pass(step, pair).wait_recv()
            send_edge(step, pair)

    def rows_of(slot):
        return pl.ds(pl.multiple_of(slot * BLOCK, BLOCK), BLOCK)

    for slot in (14, 15, 0, 1):
        place(slot)
    sides(lambda: first_right(0).start(), lambda: first_left(0).start())
    for couple in ((7, 0), (6, 1), (5, 2), (4, 3)):
        for pair in couple:
            if pair not in (0, PAIRS - 1):
                place(2 * pair)
                place(2 * pair + 1)
        send_grams(0, couple)

    def one_step(step, carry):
        solve_and_send(step)
        pass_turns(step)
        for pair in ORDER:
            take_turn(step, pair)
        for pair in ORDER:
            out = summed(turns[step, pair], buf[step, pl.ds((pair + 1) * PAIR, PAIR), :], TURN)
            top_slot, bottom_slot = 2 * pair + 4, 2 * pair + 1
            if pair == 0:
                top_slot = jnp.where(at_first, 2, top_slot)
                bottom_slot = jnp.where(at_first, 4, bottom_slot)
            if pair == PAIRS - 1:
                top_slot = jnp.where(at_last, 17, top_slot)
            buf[step + 1, rows_of(top_slot), :] = out[:BLOCK]
            buf[step + 1, rows_of(bottom_slot), :] = out[BLOCK:]
            for ready in READY.get(pair, ()):
                send_grams(step + 1, ready)

        @pl.when(step == 0)
        def _():
            sides(lambda: first_right(2).start(), lambda: first_left(2).start())

        sides(lambda: halo_right(step + 1, 0).start(), lambda: halo_left(step + 1, 0).start())

        @pl.when(has_left)
        def _():
            @pl.when(step == 0)
            def _():
                for cut in range(len(FIRST_CUTS) - 1):
                    first_right(cut).wait_recv()

            @pl.when(step > 0)
            def _():
                for cut in range(len(LATER_CUTS) - 1):
                    halo_right(step, cut).wait_recv()
            edge_right(step).wait_recv()
            buf[step + 1, pl.ds(2 * BLOCK, BLOCK), :] = summed(
                edges[step, 0], buf[step, pl.ds(0, PAIR), :], TURN
            )

        @pl.when(has_right)
        def _():
            @pl.when(step == 0)
            def _():
                for cut in range(len(FIRST_CUTS) - 1):
                    first_left(cut).wait_recv()

            @pl.when(step > 0)
            def _():
                for cut in range(len(LATER_CUTS) - 1):
                    halo_left(step, cut).wait_recv()
            edge_left(step).wait_recv()
            buf[step + 1, pl.ds(17 * BLOCK, BLOCK), :] = summed(
                edges[step, 1], buf[step, pl.ds((PAIRS + 1) * PAIR, PAIR), :], TURN
            )

        send_grams(step + 1, (PAIRS - 1, 0))
        send_grams(step + 1, (5, 2))
        send_grams(step + 1, (4, 3))
        return carry

    lax.fori_loop(0, STEPS - 1, one_step, 0)

    last = STEPS - 1
    inner = pl.ds(BLOCK, (SLOTS - 2) * BLOCK)
    store_inner = pltpu.make_async_copy(buf.at[last, inner], last_x.at[inner], out_sem.at[0])
    store_inner.start()
    solve_and_send(last)
    pass_turns(last)
    for pair in ORDER:
        take_turn(last, pair)
    store_turns = pltpu.make_async_copy(turns.at[last], last_turns, out_sem.at[1])
    store_turns.start()

    def store_side(side):
        rows = pl.ds(side * (SLOTS - 1) * BLOCK, BLOCK)
        return (
            pltpu.make_async_copy(buf.at[last, rows], last_x.at[rows], out_sem.at[2 + side]),
            pltpu.make_async_copy(edges.at[last, side], last_edges.at[side], out_sem.at[4 + side]),
        )

    @pl.when(has_left)
    def _():
        for cut in range(len(LATER_CUTS) - 1):
            halo_right(last, cut).wait_recv()
        edge_right(last).wait_recv()
        for copy in store_side(0):
            copy.start()

    @pl.when(has_right)
    def _():
        for cut in range(len(LATER_CUTS) - 1):
            halo_left(last, cut).wait_recv()
        edge_left(last).wait_recv()
        for copy in store_side(1):
            copy.start()

    def drain(step, carry):
        for pair in range(PAIRS):
            @pl.when(mine != pair)
            def _():
                gram_out(step, pair).wait_send()

            @pl.when(core == pair % 2)
            def _():
                turn_pass(step, pair).wait_send()

        swap(step).wait_send()
        for index in range(len(FAR_FIRST)):
            turn_out(step, index).wait_send()

        sides(lambda: edge_right(step).wait_send(), lambda: edge_left(step).wait_send())

        @pl.when(step > 0)
        def _():
            for cut in range(len(LATER_CUTS) - 1):
                sides(lambda: halo_right(step, cut).wait_send(), lambda: halo_left(step, cut).wait_send())
        return carry

    lax.fori_loop(0, STEPS, drain, 0)
    for cut in range(len(FIRST_CUTS) - 1):
        sides(lambda: first_right(cut).wait_send(), lambda: first_left(cut).wait_send())
    store_inner.wait()
    store_turns.wait()

    @pl.when(has_left)
    def _():
        for copy in store_side(0):
            copy.wait()

    @pl.when(has_right)
    def _():
        for copy in store_side(1):
            copy.wait()


def finish(position, x_ref, turns_ref, edges_ref, out_ref):
    at_first = position[0] == 0
    at_last = position[0] == COLS - 1

    def put(slot, value):
        out_ref[slot * BLOCK : (slot + 1) * BLOCK, :] = value

    for pair in range(PAIRS):
        out = summed(turns_ref[pair], x_ref[(pair + 1) * PAIR : (pair + 2) * PAIR, :], ROUGH)
        top, bottom = out[:BLOCK], out[BLOCK:]
        if pair == 0:
            left = summed(edges_ref[0], x_ref[:PAIR, :], ROUGH)
            put(0, jnp.where(at_first, top, left))
            put(2, jnp.where(at_first, bottom, top))
        elif pair == PAIRS - 1:
            right = summed(edges_ref[1], x_ref[(PAIRS + 1) * PAIR :, :], ROUGH)
            put(2 * pair - 1, bottom)
            put(2 * pair + 1, jnp.where(at_last, top, right))
        else:
            put(2 * pair - 1, bottom)
            put(2 * pair + 2, top)


def local(columns, block_order):
    length = columns.shape[1]
    blocks = columns.reshape(2 * PAIRS, BLOCK, length)
    dma = pltpu.SemaphoreType.DMA
    position = lax.axis_index("col").astype(jnp.int32).reshape(1)
    last_x, last_turns, last_edges = pl.pallas_call(
        sweep,
        out_shape=(
            jax.ShapeDtypeStruct((SLOTS * BLOCK, length), jnp.float32),
            jax.ShapeDtypeStruct((PAIRS, PAIR, PAIR), jnp.float32),
            jax.ShapeDtypeStruct((2, BLOCK, PAIR), jnp.float32),
        ),
        in_specs=[
            pl.BlockSpec(memory_space=pltpu.SMEM),
            pl.BlockSpec(memory_space=pl.ANY),
        ],
        out_specs=(pl.BlockSpec(memory_space=pl.ANY),) * 3,
        scratch_shapes=[
            pltpu.VMEM(blocks.shape, jnp.float32),
            pltpu.VMEM((STEPS, SLOTS * BLOCK, length), jnp.float32),
            pltpu.VMEM((STEPS, PAIRS, MESSAGE, PAIR), jnp.float32),
            pltpu.VMEM((STEPS, PAIRS, MESSAGE, PAIR), jnp.float32),
            pltpu.VMEM((STEPS, MESSAGE, PAIR), jnp.float32),
            pltpu.VMEM((STEPS, MESSAGE, PAIR), jnp.float32),
            pltpu.VMEM((STEPS, PAIRS, PAIR, PAIR), jnp.float32),
            pltpu.VMEM((STEPS, 2, BLOCK, PAIR), jnp.float32),
            dma,
            dma((6,)),
            dma((STEPS, PAIRS)),
            dma((STEPS, PAIRS)),
            dma((STEPS,)),
            dma((STEPS,)),
            dma((STEPS, len(FAR_FIRST))),
            dma((STEPS, PAIRS)),
            dma((STEPS, PAIRS)),
            dma((STEPS, 2)),
            dma((STEPS, 2)),
            dma((2, len(FIRST_CUTS) - 1)),
            dma((2, len(FIRST_CUTS) - 1)),
            dma((STEPS, 2 * len(LATER_CUTS) - 2)),
            dma((STEPS, 2 * len(LATER_CUTS) - 2)),
        ],
        compiler_params=pltpu.CompilerParams(
            collective_id=0, has_side_effects=True, vmem_limit_bytes=58 * 1024 * 1024
        ),
    )(block_order, blocks)
    wide = 512
    return pl.pallas_call(
        finish,
        grid=(length // wide,),
        out_shape=jax.ShapeDtypeStruct(columns.shape, jnp.float32),
        in_specs=[
            pl.BlockSpec(memory_space=pltpu.SMEM),
            pl.BlockSpec((SLOTS * BLOCK, wide), lambda part: (0, part)),
            pl.BlockSpec((PAIRS, PAIR, PAIR), lambda part: (0, 0, 0)),
            pl.BlockSpec((2, BLOCK, PAIR), lambda part: (0, 0, 0)),
        ],
        out_specs=pl.BlockSpec((columns.shape[0], wide), lambda part: (0, part)),
    )(position, last_x, last_turns, last_edges)


def solution(mesh):
    placed = (P("col", "row"), P("col"))
    return jax.shard_map(
        local, mesh=mesh, in_specs=placed, out_specs=P("col", "row"), check_vma=False
    )
```
